16 devices in a mesh: dp: 4 (over z, y), tp: 4 (over x, core).
Axes of the slice: x: 2, y: 2, z: 2, core: 2. Of those that a mesh axis runs over, the one named last changes fastest.
Arguments:
- tokens: bfloat16 [4, 6144, 3072], P('dp', 'tp'), parts along dimension 0
- cond_vec: float32 [4, 3072], P('dp'), parts along dimension 0
- txt_len: int32 [4], P('dp'), parts along dimension 0
- grid_hw: int32 [4, 2], P('dp'), parts along dimension 0
- w_mod: bfloat16 [3072, 9216], replicated
- b_mod: float32 [9216], replicated
- w_qkv: bfloat16 [3072, 3, 3072], P(None, None, 'tp')
- b_qkv: float32 [3, 3072], P(None, 'tp')
- q_gain: float32 [128], replicated
- k_gain: float32 [128], replicated
- w_mlp_in: bfloat16 [3072, 12288], P(None, 'tp')
- b_mlp_in: float32 [12288], P('tp')
- w_out_attn: bfloat16 [3072, 3072], P('tp')
- w_out_mlp: bfloat16 [12288, 3072], P('tp')
- b_out: float32 [3072], replicated
Outputs:
- output: bfloat16 [4, 6144, 3072], P('dp', 'tp'), parts along dimension 0
There are 4 independent parts. The reference program is written for one: setup_inputs(seed, part) draws one part's arguments, and reference() takes and returns one part's arrays. A program takes and returns all parts, laid end to end along the dimension named above; an argument that names none is the same for every part.
All inputs are finite; a program needn't handle non-finite values.
Results may differ from the reference program's by a relative error of at most 0.00356712.
Values are sent between devices in bfloat16 or wider.
A program may use at most 1 GiB of HBM per device.

```python
import jax
import jax.numpy as jnp
from jax import lax

BATCH = 1
SEQ = 6144
D = 3072
HEADS = 24
HEAD = 128
FF = 12288
TXT = 256
QBLOCK = 256
GRID_MIN = 16
GRID_MAX = 96
VID = SEQ - TXT
EPS = 1e-6
THETA = 256.0


def setup_inputs(seed: int = 0, part: int = 0) -> dict:
    part_key = jax.random.fold_in(jax.random.key(seed), part)
    act_keys = jax.random.split(part_key, 2)
    int_keys = jax.random.split(jax.random.fold_in(part_key, 1), 3)
    w_keys = jax.random.split(jax.random.key(seed + 1), 11)
    tokens = jax.random.normal(act_keys[0], (BATCH, SEQ, D), jnp.float32).astype(jnp.bfloat16)
    cond_vec = jax.random.normal(act_keys[1], (BATCH, D), jnp.float32)
    sample_idx = jnp.arange(BATCH)
    low_len = jax.random.randint(int_keys[0], (BATCH,), TXT // 8, TXT // 2)
    high_len = jax.random.randint(int_keys[1], (BATCH,), TXT // 2, TXT + 1)
    txt_len = jnp.where(sample_idx % 2 == 0, low_len, high_len)
    txt_len = jnp.where(sample_idx == max(BATCH - 1, 1), TXT, txt_len).astype(jnp.int32)
    grid_hw = jax.random.randint(int_keys[2], (BATCH, 2), GRID_MIN, GRID_MAX + 1)
    first_h = (sample_idx[:, None] == 0) & (jnp.arange(2)[None, :] == 0)
    grid_hw = jnp.where(first_h, GRID_MAX, grid_hw).astype(jnp.int32)
    d_scale = D ** -0.5
    out_scale = (D + FF) ** -0.5
    gate_offset = jnp.where(jnp.arange(3 * D) >= 2 * D, 1.0, 0.0)
    return {
        'tokens': tokens,
        'cond_vec': cond_vec,
        'txt_len': txt_len,
        'grid_hw': grid_hw,
        'w_mod': (jax.random.normal(w_keys[0], (D, 3 * D), jnp.float32) * d_scale).astype(jnp.bfloat16),
        'b_mod': 0.5 * jax.random.normal(w_keys[1], (3 * D,), jnp.float32) + gate_offset,
        'w_qkv': (jax.random.normal(w_keys[2], (D, 3, D), jnp.float32) * d_scale).astype(jnp.bfloat16),
        'b_qkv': 0.3 * jax.random.normal(w_keys[3], (3, D), jnp.float32),
        'q_gain': 1.6 + 0.3 * jax.random.normal(w_keys[4], (HEAD,), jnp.float32),
        'k_gain': 1.6 + 0.3 * jax.random.normal(w_keys[5], (HEAD,), jnp.float32),
        'w_mlp_in': (jax.random.normal(w_keys[6], (D, FF), jnp.float32) * d_scale).astype(jnp.bfloat16),
        'b_mlp_in': 0.3 * jax.random.normal(w_keys[7], (FF,), jnp.float32),
        'w_out_attn': (jax.random.normal(w_keys[8], (D, D), jnp.float32) * out_scale).astype(jnp.bfloat16),
        'w_out_mlp': (jax.random.normal(w_keys[9], (FF, D), jnp.float32) * out_scale).astype(jnp.bfloat16),
        'b_out': 0.3 * jax.random.normal(w_keys[10], (D,), jnp.float32),
    }


def rope_table(grid_hw):
    tok_idx = jnp.arange(SEQ, dtype=jnp.int32)[None, :]
    grid_h = grid_hw[:, 0:1]
    grid_w = grid_hw[:, 1:2]
    t_pos = tok_idx // (grid_h * grid_w)
    h_pos = (tok_idx // grid_w) % grid_h
    w_pos = tok_idx % grid_w
    pair_idx = jnp.arange(HEAD // 2, dtype=jnp.int32)
    axis_sel = (pair_idx >= 8).astype(jnp.int32) + (pair_idx >= 36).astype(jnp.int32)
    within = pair_idx - jnp.where(axis_sel == 0, 0, jnp.where(axis_sel == 1, 8, 36))
    axis_dim = jnp.where(axis_sel == 0, 16.0, 56.0)
    inv_freq = jnp.power(THETA, -2.0 * within.astype(jnp.float32) / axis_dim)
    pos_sel = jnp.where(axis_sel == 0, t_pos[..., None], jnp.where(axis_sel == 1, h_pos[..., None], w_pos[..., None]))
    angles = pos_sel.astype(jnp.float32) * inv_freq
    angles = jnp.where((tok_idx < VID)[..., None], angles, 0.0)
    return jnp.cos(angles), jnp.sin(angles)


def apply_rope(heads_f32, cos_t, sin_t):
    full_shape = heads_f32.shape
    pairs = heads_f32.reshape(full_shape[:-1] + (full_shape[-1] // 2, 2))
    real_part = pairs[..., 0]
    imag_part = pairs[..., 1]
    cos_b = cos_t[:, :, None, :]
    sin_b = sin_t[:, :, None, :]
    rotated = jnp.stack([real_part * cos_b - imag_part * sin_b, real_part * sin_b + imag_part * cos_b], axis=-1)
    return rotated.reshape(full_shape)


def head_rms(heads_f32, gain):
    mean_sq = jnp.mean(heads_f32 * heads_f32, axis=-1, keepdims=True)
    return heads_f32 * lax.rsqrt(mean_sq + EPS) * gain


def attention(q_heads, k_heads, v_heads, tok_valid):
    qk_scale = HEAD ** -0.5
    def one_sample(sample):
        q_one, k_one, v_one, valid_one = sample
        keys_f32 = k_one.astype(jnp.float32)
        vals_f32 = v_one.astype(jnp.float32)
        def one_block(block_id):
            q_blk = lax.dynamic_slice_in_dim(q_one, block_id * QBLOCK, QBLOCK, axis=0).astype(jnp.float32)
            q_valid = lax.dynamic_slice_in_dim(valid_one, block_id * QBLOCK, QBLOCK, axis=0)
            same_seg = q_valid[:, None] == valid_one[None, :]
            scores = jnp.einsum('qhd,khd->hqk', q_blk, keys_f32) * qk_scale
            scores = jnp.where(same_seg[None, :, :], scores, -1e30)
            probs = jax.nn.softmax(scores, axis=-1).astype(jnp.bfloat16).astype(jnp.float32)
            return jnp.einsum('hqk,khd->qhd', probs, vals_f32).astype(jnp.bfloat16)
        blocks = lax.map(one_block, jnp.arange(SEQ // QBLOCK))
        return blocks.reshape(SEQ, HEADS, HEAD)
    return lax.map(one_sample, (q_heads, k_heads, v_heads, tok_valid))


def reference(tokens, cond_vec, txt_len, grid_hw, w_mod, b_mod, w_qkv, b_qkv, q_gain, k_gain, w_mlp_in, b_mlp_in, w_out_attn, w_out_mlp, b_out):
    mod_all = jnp.dot(jax.nn.silu(cond_vec).astype(jnp.bfloat16), w_mod, preferred_element_type=jnp.float32) + b_mod
    shift = mod_all[:, :D]
    scale = mod_all[:, D:2 * D]
    gate = mod_all[:, 2 * D:]
    tok_f32 = tokens.astype(jnp.float32)
    centered = tok_f32 - jnp.mean(tok_f32, axis=-1, keepdims=True)
    variance = jnp.mean(centered * centered, axis=-1, keepdims=True)
    normed = centered * lax.rsqrt(variance + EPS)
    y_mod = (normed * (1.0 + scale[:, None, :]) + shift[:, None, :]).astype(jnp.bfloat16)
    y_rows = y_mod.reshape(BATCH * SEQ, D)
    qkv_f32 = jnp.dot(y_rows, w_qkv.reshape(D, 3 * D), preferred_element_type=jnp.float32).reshape(BATCH, SEQ, 3, D) + b_qkv
    cos_t, sin_t = rope_table(grid_hw)
    head_shape = (BATCH, SEQ, HEADS, HEAD)
    q_heads = apply_rope(head_rms(qkv_f32[:, :, 0].reshape(head_shape), q_gain), cos_t, sin_t).astype(jnp.bfloat16)
    k_heads = apply_rope(head_rms(qkv_f32[:, :, 1].reshape(head_shape), k_gain), cos_t, sin_t).astype(jnp.bfloat16)
    v_heads = qkv_f32[:, :, 2].reshape(head_shape).astype(jnp.bfloat16)
    tok_valid = jnp.arange(SEQ)[None, :] < (VID + txt_len)[:, None]
    attended = attention(q_heads, k_heads, v_heads, tok_valid).reshape(BATCH * SEQ, D)
    mlp_pre = jnp.dot(y_rows, w_mlp_in, preferred_element_type=jnp.float32) + b_mlp_in
    mlp_act = jax.nn.gelu(mlp_pre, approximate=True).astype(jnp.bfloat16)
    projected = jnp.dot(attended, w_out_attn, preferred_element_type=jnp.float32) + jnp.dot(mlp_act, w_out_mlp, preferred_element_type=jnp.float32) + b_out
    result = tok_f32 + gate[:, None, :] * projected.reshape(BATCH, SEQ, D)
    return result.astype(jnp.bfloat16)
```

```python
import functools
import jax
import jax.numpy as jnp
from jax import lax
from jax.experimental import pallas as pl
from jax.experimental.pallas import tpu as pltpu
from jax.sharding import PartitionSpec as P


SEQ = 6144
D = 3072
HD = 128
TXT = 256
VID = SEQ - TXT
EPS = 1e-6
THETA = 256.0
SHARD = 1536
CHIP = 2 * SHARD
DQ = 768
LOG2E = 1.4426950408889634
BF = jnp.bfloat16
F32 = jnp.float32
NT = (((1,), (1,)), ((), ()))
X_PAIRS = [(0, 2), (1, 3), (2, 0), (3, 1)]
C_PAIRS = [(0, 1), (1, 0), (2, 3), (3, 2)]


def params(mib=60, **kw):
    return pltpu.CompilerParams(vmem_limit_bytes=mib * 2 ** 20, **kw)


def cost(flops, nbytes):
    return pl.CostEstimate(flops=int(flops), bytes_accessed=int(nbytes), transcendentals=0)


def norm_kernel(x_ref, scale_ref, shift_ref, y_ref):
    x = x_ref[...].astype(F32)
    c = x - jnp.mean(x, axis=-1, keepdims=True)
    var = jnp.mean(c * c, axis=-1, keepdims=True)
    y_ref[...] = (c * lax.rsqrt(var + EPS) * scale_ref[...] + shift_ref[...]).astype(BF)


def norm(x, scale1, shift):
    bm = 256
    n = x.shape[0]
    row = pl.BlockSpec((1, D), lambda i: (0, 0))
    blk = pl.BlockSpec((bm, D), lambda i: (i, 0))
    return pl.pallas_call(norm_kernel, grid=(n // bm,), in_specs=[blk, row, row], out_specs=blk,
                          out_shape=jax.ShapeDtypeStruct((n, D), BF), compiler_params=params(),
                          cost_estimate=cost(n * D * 8, n * D * 4), name="norm")(x, scale1, shift)


QBM = 512
SUB = 256


def qkv_kernel(half, off_ref, y0_ref, y1_ref, w_ref, b_ref, qg_ref, kg_ref, cos_ref, sin_ref, *refs):
    q_ref, k_ref, vt_ref, left0, left1 = refs[-5:]
    n = pl.program_id(1)
    tiles = [(i, s) for i in range(QBM // SUB) for s in range(DQ // SUB)]
    pairs = [tiles[a:a + 2] for a in range(0, len(tiles), 2)]

    def proj(y_ref, t):
        return jnp.dot(y_ref[pl.ds(t[0] * SUB, SUB), :], w_ref[0, :, pl.ds(t[1] * SUB, SUB)], preferred_element_type=F32)

    def rope(r, t, gain_ref, row, out_ref):
        at = pl.ds(t[0] * SUB, SUB)
        even = lax.broadcasted_iota(jnp.int32, (SUB, HD), 1) % 2 == 0
        for h in range(SUB // HD):
            lo = t[1] * SUB + h * HD
            x = r[:, h * HD:(h + 1) * HD] + b_ref[row:row + 1, lo:lo + HD]
            ms = jnp.mean(x * x, axis=-1, keepdims=True)
            x = x * lax.rsqrt(ms + EPS) * gain_ref[...]
            partner = jnp.where(even, pltpu.roll(x, HD - 1, 1), pltpu.roll(x, 1, 1))
            out_ref[at, lo:lo + HD] = (x * cos_ref[at, :] + partner * sin_ref[at, :]).astype(BF)

    def put(r, t):
        lo = t[1] * SUB
        vt_ref[pl.ds(lo, SUB), pl.ds(t[0] * SUB, SUB)] = (r + b_ref[2:3, lo:lo + SUB]).T.astype(BF)

    def q_epi(r, t):
        rope(r, t, qg_ref, 0, q_ref)

    def k_epi(r, t):
        rope(r, t, kg_ref, 1, k_ref)

    def run(y_ref, epi, before, keep):
        held = []
        for p, pair in enumerate(pairs):
            last = keep and p == len(pairs) - 1
            now = [(proj(y_ref, t), t) for t in pair]
            if last:
                left0[...] = now[0][0]
                left1[...] = now[1][0]
            if p == 0 and before is not None:
                before(left0[...], pairs[-1][0])
                before(left1[...], pairs[-1][1])
            for r, t in held:
                epi(r, t)
            held = [] if last else now
        for r, t in held:
            epi(r, t)

    def step(y_ref):
        @pl.when(n == 0)
        def _():
            run(y_ref, q_epi, None, True)

        @pl.when(n == 1)
        def _():
            run(y_ref, k_epi, q_epi, True)

        @pl.when(n == 2)
        def _():
            run(y_ref, put, k_epi, False)

    if half is None:
        step(y0_ref)
    else:
        @pl.when(pl.program_id(0) < half)
        def _():
            step(y0_ref)

        @pl.when(pl.program_id(0) >= half)
        def _():
            step(y1_ref)


def qkv(off, ys, w3, b, qg, kg, cos, sin, prev=None):
    m0 = ys[0].shape[0] // QBM
    half = m0 if len(ys) == 2 else None
    m = m0 * len(ys)
    at = lambda i, o: jnp.where(i < m0, o[0] + i, o[1] + i - m0)
    in_specs = [pl.BlockSpec((QBM, D), lambda i, n, o: (jnp.minimum(i, m0 - 1), 0)),
                pl.BlockSpec((QBM, D), (lambda i, n, o: (jnp.maximum(i - m0, 0), 0)) if half else (lambda i, n, o: (0, 0))),
                pl.BlockSpec((1, D, DQ), lambda i, n, o: (n, 0, 0)),
                pl.BlockSpec((3, DQ), lambda i, n, o: (0, 0)),
                pl.BlockSpec((1, HD), lambda i, n, o: (0, 0)),
                pl.BlockSpec((1, HD), lambda i, n, o: (0, 0)),
                pl.BlockSpec((QBM, HD), lambda i, n, o: (at(i, o), 0)),
                pl.BlockSpec((QBM, HD), lambda i, n, o: (at(i, o), 0))]
    args = [off, ys[0], ys[-1], w3, b, qg, kg, cos, sin]
    if half is None:
        in_specs[1] = pl.BlockSpec(memory_space=pl.ANY)
    alias = {}
    if prev is not None:
        in_specs += [pl.BlockSpec(memory_space=pl.ANY)] * 3
        args += list(prev)
        alias = {9: 0, 10: 1, 11: 2}
    return pl.pallas_call(
        functools.partial(qkv_kernel, half),
        grid_spec=pltpu.PrefetchScalarGridSpec(
            num_scalar_prefetch=1, grid=(m, 3), in_specs=in_specs,
            out_specs=[pl.BlockSpec((QBM, DQ), lambda i, n, o: (at(i, o), 0)),
                       pl.BlockSpec((QBM, DQ), lambda i, n, o: (at(i, o), 0)),
                       pl.BlockSpec((DQ, QBM), lambda i, n, o: (0, at(i, o)))],
            scratch_shapes=[pltpu.VMEM((SUB, SUB), F32)] * 2),
        out_shape=[jax.ShapeDtypeStruct((SEQ, DQ), BF), jax.ShapeDtypeStruct((SEQ, DQ), BF),
                   jax.ShapeDtypeStruct((DQ, SEQ), BF)],
        input_output_aliases=alias, compiler_params=params(),
        cost_estimate=cost(2 * m * QBM * D * 3 * DQ, m * QBM * D * 2 + 3 * D * DQ * 2), name="qkv")(*args)


BQ = 1536
BK = 512


def attn_kernel(sc_ref, q_ref, k_ref, vt_ref, o_ref, flag_ref):
    i = pl.program_id(1)
    txt_len = sc_ref[1]

    @pl.when(i == 0)
    def _():
        vmax = jnp.max(jnp.abs(vt_ref[...].astype(F32)))
        flag_ref[0] = jnp.logical_and(vmax <= 4096.0, sc_ref[2] == 1).astype(jnp.int32)

    bq = q_ref.shape[0]
    nk = SEQ // BK
    last = BK - TXT
    first_row = (sc_ref[0] + i) * bq
    has_pad = jnp.logical_and(first_row + bq == SEQ, txt_len < TXT)

    def scores(j):
        return lax.dot_general(k_ref[pl.ds(j * BK, BK), :], q_ref[...], NT, preferred_element_type=F32)

    def key_ok():
        return lax.broadcasted_iota(jnp.int32, (BK, 1), 0) < last + txt_len

    def finish(acc, l):
        o = acc * (1.0 / l)
        o_ref[...] = o.T.astype(BF)

        @pl.when(has_pad)
        def _():
            s = lax.dot_general(k_ref[pl.ds(VID, TXT), :], q_ref[...], NT, preferred_element_type=F32)
            pad_key = lax.broadcasted_iota(jnp.int32, (TXT, 1), 0) >= txt_len
            s = jnp.where(pad_key, s, -1e30)
            p = jnp.exp2(s - jnp.max(s, axis=0, keepdims=True))
            lp = jnp.sum(p, axis=0, keepdims=True)
            ap = jnp.dot(vt_ref[:, pl.ds(VID, TXT)], p.astype(BF), preferred_element_type=F32)
            row = first_row + lax.broadcasted_iota(jnp.int32, (bq, 1), 0)
            o_ref[...] = jnp.where(row < VID + txt_len, o_ref[...].astype(F32), (ap * (1.0 / lp)).T).astype(BF)

    @pl.when(flag_ref[0] == 1)
    def _():
        acc = jnp.zeros((HD, bq), F32)
        l = jnp.zeros((1, bq), F32)
        s = scores(0)
        for j in range(nk):
            nxt = scores(j + 1) if j + 1 < nk else None
            p = jnp.exp2(s)
            if j == nk - 1:
                p = jnp.where(key_ok(), p, 0.0)
            l = l + jnp.sum(p, axis=0, keepdims=True)
            acc = acc + jnp.dot(vt_ref[:, pl.ds(j * BK, BK)], p.astype(BF), preferred_element_type=F32)
            s = nxt
        finish(acc, l)

    @pl.when(flag_ref[0] == 0)
    def _():
        def step(j, carry):
            m, l, acc = carry
            at = pl.multiple_of(j * BK, BK)
            s = lax.dot_general(k_ref[pl.ds(at, BK), :], q_ref[...], NT, preferred_element_type=F32)
            s = jnp.where(jnp.logical_or(key_ok(), j < nk - 1), s, -1e30)
            mn = jnp.maximum(m, jnp.max(s, axis=0, keepdims=True))
            p = jnp.exp2(s - mn)
            a = jnp.exp2(m - mn)
            l = l * a + jnp.sum(p, axis=0, keepdims=True)
            acc = acc * a + jnp.dot(vt_ref[:, pl.ds(at, BK)], p.astype(BF), preferred_element_type=F32)
            return mn, l, acc

        init = (jnp.full((1, bq), -1e30, F32), jnp.zeros((1, bq), F32), jnp.zeros((HD, bq), F32))
        _, l, acc = lax.fori_loop(0, nk, step, init)
        finish(acc, l)


def attend(scalars, q, k, vt, rows, h0, nh):
    nb = rows // BQ
    return pl.pallas_call(
        attn_kernel,
        grid_spec=pltpu.PrefetchScalarGridSpec(
            num_scalar_prefetch=1, grid=(nh, nb),
            in_specs=[pl.BlockSpec((BQ, HD), lambda h, i, s: (s[0] + i, h0 + h)),
                      pl.BlockSpec((SEQ, HD), lambda h, i, s: (0, h0 + h)),
                      pl.BlockSpec((HD, SEQ), lambda h, i, s: (h0 + h, 0))],
            out_specs=pl.BlockSpec((BQ, HD), lambda h, i, s: (i, h)),
            scratch_shapes=[pltpu.SMEM((1,), jnp.int32)]),
        out_shape=jax.ShapeDtypeStruct((rows, nh * HD), BF), compiler_params=params(),
        cost_estimate=cost(6 * rows * SEQ * nh * HD, 4 * nh * HD * (SEQ + rows)), name="attend")(scalars, q, k, vt)


def gelu_kernel(half, nw, off_ref, y0_ref, y1_ref, *refs):
    w_refs, b_ref, o_ref = refs[:len(refs) - 2], refs[-2], refs[-1]
    bn = o_ref.shape[1]
    i = pl.program_id(0)
    j = pl.program_id(1)
    sub = 512 if bn % 512 == 0 else 768

    def step(y_ref, w_ref):
        for s in range(bn // sub):
            u = jnp.dot(y_ref[...], w_ref[:, pl.ds(s * sub, sub)], preferred_element_type=F32)
            u = u + b_ref[:, pl.ds(s * sub, sub)]
            h = 0.5 * u
            t = jnp.tanh(u * (0.7978845608028654 + 0.03567740813636141 * (u * u)))
            o_ref[:, pl.ds(s * sub, sub)] = (h * t + h).astype(BF)

    for a, y_ref in enumerate((y0_ref, y1_ref)):
        for c, w_ref in enumerate(w_refs):
            hit = (i < half) if a == 0 else (i >= half)
            if len(w_refs) > 1:
                hit = jnp.logical_and(hit, j // nw == c)

            @pl.when(hit)
            def _(y_ref=y_ref, w_ref=w_ref):
                step(y_ref, w_ref)


def mlp_in(off, ys, ws, b):
    n = ys[0].shape[0]
    f = sum(w.shape[1] for w in ws)
    bm = 768
    bn = 1024 if len(ws) == 1 else 768
    nw = ws[0].shape[1] // bn
    half = n // bm
    at = lambda i, o: jnp.where(i < half, o[0] + i, o[1] + i - half)
    wspec = lambda c: pl.BlockSpec((D, bn), lambda i, j, o: (0, jnp.clip(j - c * nw, 0, nw - 1)))
    return pl.pallas_call(
        functools.partial(gelu_kernel, half, nw),
        grid_spec=pltpu.PrefetchScalarGridSpec(
            num_scalar_prefetch=1, grid=(2 * half, f // bn),
            in_specs=[pl.BlockSpec((bm, D), lambda i, j, o: (jnp.minimum(i, half - 1), 0)),
                      pl.BlockSpec((bm, D), lambda i, j, o: (jnp.maximum(i - half, 0), 0))]
            + [wspec(c) for c in range(len(ws))] + [pl.BlockSpec((1, bn), lambda i, j, o: (0, j))],
            out_specs=pl.BlockSpec((bm, bn), lambda i, j, o: (at(i, o), j))),
        out_shape=jax.ShapeDtypeStruct((2 * n, f), BF),
        compiler_params=params(), cost_estimate=cost(4 * n * D * f, n * D * 4 + D * f * 2 + n * f * 4), name="mlp_in")(off, *ys, *ws, b)


def mm_kernel(x_ref, w_ref, o_ref):
    o_ref[...] = jnp.dot(x_ref[...], w_ref[...], preferred_element_type=F32)


def mm_f32(x, w):
    n, kd, f = x.shape[0], x.shape[1], w.shape[1]
    bm = bn = 1024
    return pl.pallas_call(
        mm_kernel, grid=(n // bm, f // bn),
        in_specs=[pl.BlockSpec((bm, kd), lambda i, j: (i, 0)), pl.BlockSpec((kd, bn), lambda i, j: (0, j))],
        out_specs=pl.BlockSpec((bm, bn), lambda i, j: (i, j)), out_shape=jax.ShapeDtypeStruct((n, f), F32),
        compiler_params=params(), cost_estimate=cost(2 * n * kd * f, n * kd * 2 + kd * f * 2 + n * f * 4), name="mlp_out")(x, w)


def out_kernel(final, off_ref, *refs):
    m_ref, wm0_ref, wm1_ref, a0_ref, a1_ref, b_ref, w0_ref, w1_ref, p_ref = refs[:9]
    o_ref = refs[-1]
    hk = wm0_ref.shape[0]
    dot = lambda a, w: jnp.dot(a, w, preferred_element_type=F32)
    acc = dot(m_ref[:, :hk], wm0_ref[...]) + dot(m_ref[:, hk:], wm1_ref[...])
    acc = acc + dot(a0_ref[...], w0_ref[...])
    acc = acc + dot(jnp.concatenate([a1_ref[...], b_ref[...]], axis=1), w1_ref[...])
    acc = acc + p_ref[...]
    if final:
        recv_ref, x_ref, gate_ref, bo_ref = refs[9:13]
        acc = x_ref[...].astype(F32) + gate_ref[...] * (acc + recv_ref[...] + bo_ref[...])
    o_ref[...] = acc.astype(o_ref.dtype)


def out_rows(off, n, m, wms, a0, a1s, w0, w1, part, tail=None):
    bm, bn = 768, 768
    f = D
    rowk = lambda kd: pl.BlockSpec((bm, kd), lambda i, j, o: (o[0] + i, 0))
    col = lambda kd: pl.BlockSpec((kd, bn), lambda i, j, o: (0, j))
    in_specs = [rowk(D), col(D // 2), col(D // 2), pl.BlockSpec((bm, DQ), lambda i, j, o: (i, 0)), rowk(DQ // 2), rowk(DQ // 2), col(DQ), col(DQ),
                pl.BlockSpec((bm, bn), lambda i, j, o: (o[0] + i, j))]
    args = [off, m, *wms, a0, *a1s, w0, w1, part]
    if tail is not None:
        tile = pl.BlockSpec((bm, bn), lambda i, j, o: (i, j))
        vec = pl.BlockSpec((1, bn), lambda i, j, o: (0, j))
        in_specs += [tile, tile, vec, vec]
        args += list(tail)
    dt = BF if tail is not None else F32
    return pl.pallas_call(
        functools.partial(out_kernel, tail is not None),
        grid_spec=pltpu.PrefetchScalarGridSpec(num_scalar_prefetch=1, grid=(n // bm, f // bn), in_specs=in_specs,
            out_specs=pl.BlockSpec((bm, bn), lambda i, j, o: (i, j))),
        out_shape=jax.ShapeDtypeStruct((n, f), dt), compiler_params=params(),
        cost_estimate=cost(2 * n * (D + 2 * DQ) * f, n * D * 14), name="out_rows")(*args)


def modulation(cond_vec, w_mod, b_mod):
    return jnp.dot(jax.nn.silu(cond_vec).astype(BF), w_mod, preferred_element_type=F32) + b_mod


def rope_table(grid_hw):
    n = lax.broadcasted_iota(jnp.int32, (SEQ, HD), 0)
    lane = lax.broadcasted_iota(jnp.int32, (SEQ, HD), 1)
    tok = lax.iota(jnp.int32, SEQ)
    gh = grid_hw[0, 0]
    gw = grid_hw[0, 1]
    t = (tok // (gh * gw)).astype(F32)
    r = ((tok // gw) % gh).astype(F32)
    c = (tok % gw).astype(F32)
    pair = lax.iota(jnp.int32, HD) // 2
    axis = (pair >= 8).astype(jnp.int32) + (pair >= 36).astype(jnp.int32)
    within = pair - jnp.where(axis == 0, 0, jnp.where(axis == 1, 8, 36))
    dim = jnp.where(axis == 0, 16.0, 56.0)
    freq = jnp.power(THETA, -2.0 * within.astype(F32) / dim)
    pos = jnp.where(axis[None] == 0, t[:, None], jnp.where(axis[None] == 1, r[:, None], c[:, None]))
    ang = jnp.where((tok < VID)[:, None], pos * freq[None], 0.0)
    sign = jnp.where(lax.iota(jnp.int32, HD) % 2 == 0, -1.0, 1.0)
    return jnp.cos(ang), jnp.sin(ang) * sign[None]


def pair_max(g):
    a = jnp.abs(g).reshape(HD // 2, 2)
    return jnp.max(a, axis=1)


def after(v, *deps):
    return lax.optimization_barrier((v,) + deps)[0]


def solution(mesh):
    def local_step(tokens, cond_vec, txt_len, grid_hw, w_mod, b_mod, w_qkv, b_qkv, q_gain, k_gain,
                   w_mlp_in, b_mlp_in, w_out_attn, w_out_mlp, b_out):
        tp = lax.axis_index('tp')
        dp = lax.axis_index('dp')
        chip = tp // 2
        own = tp % 2
        x = tokens[0]

        def swap_x(v):
            return lax.ppermute(v, 'tp', X_PAIRS)

        def swap_c(v):
            return lax.ppermute(v, 'tp', C_PAIRS)

        gather = lambda v: lax.all_gather(v, 'dp', axis=0, tiled=True)
        vec2 = lambda a, b: jnp.stack([a, b]).astype(jnp.int32)
        vec1 = lambda a: jnp.reshape(a, (1,)).astype(jnp.int32)

        q4 = D // 4
        hop_in = [swap_x(lax.dynamic_slice(w_mlp_in, (dp * q4, c * (D // 2)), (q4, D // 2))) for c in range(2)]
        hop_att = swap_x(lax.dynamic_slice_in_dim(w_out_attn, dp * (DQ // 4), DQ // 4, 0))
        hop_out = [swap_x(lax.dynamic_slice_in_dim(w_out_mlp, c * (D // 2) + dp * (D // 8), D // 8, 0)) for c in range(2)]
        b_in_o = swap_x(b_mlp_in)[None]

        mod = modulation(cond_vec, w_mod, b_mod)
        shift, scale, gate = mod[:, :D], mod[:, D:2 * D], mod[:, 2 * D:]
        y = norm(x, 1.0 + scale, shift)
        y_sib = swap_c(y)
        y_rem = swap_x(y)

        cos, sin = rope_table(grid_hw)
        w3 = jnp.transpose(w_qkv, (1, 0, 2))
        qg = (q_gain * (LOG2E * HD ** -0.5))[None]
        kg = k_gain[None]
        nb = SHARD // QBM
        sib = tp + 1 - 2 * own
        rem = (tp + 2) % 4
        remsib = (sib + 2) % 4
        tabs = (w3, b_qkv, qg, kg, cos, sin)
        rows2 = vec2(own * 2, 2 - own * 2)

        bufs = qkv(vec2(tp * nb, tp * nb), [y], *tabs)
        w_in_o0 = gather(after(hop_in[0], bufs[0]))
        m_own = mlp_in(rows2, [y, y_sib], [w_mlp_in], b_mlp_in[None])
        w_in_o1 = gather(after(hop_in[1], m_own))
        bufs = qkv(vec2(sib * nb, sib * nb), [y_sib], *tabs, bufs)
        part = mm_f32(m_own, w_out_mlp)
        w_att_o = gather(after(hop_att, part))
        m_oth = mlp_in(rows2, [y, y_sib], [w_in_o0, w_in_o1], b_in_o)
        y_rem = after(y_rem, m_oth)
        y_remsib = swap_c(y_rem)
        bufs = qkv(vec2(rem * nb, rem * nb), [y_rem], *tabs, bufs)
        w_out_o0 = gather(after(hop_out[0], bufs[0]))
        q, k, vt = qkv(vec2(remsib * nb, remsib * nb), [y_remsib], *tabs, bufs)

        gmax = jnp.max(pair_max(q_gain) * pair_max(k_gain)) * (HD ** 0.5 * LOG2E)
        ok = (gmax <= 96.0).astype(jnp.int32)
        sc = lambda b: jnp.stack([b, txt_len[0], ok]).astype(jnp.int32)
        att_r0 = attend(sc((1 - chip) * 2), q, k, vt, CHIP, 0, 3)
        att_b0 = swap_x(att_r0)
        w_out_o1 = gather(after(hop_out[1], att_r0))
        att_r1 = attend(after(sc((1 - chip) * 2), att_r0), q, k, vt, CHIP, 3, 3)
        att_b1 = swap_x(att_r1)
        att_s = attend(after(sc(sib), att_r1), q, k, vt, SHARD, 0, 6)

        weights = (w_out_attn, w_att_o)
        sib_part = out_rows(vec1((1 - own) * 2), SHARD, m_oth, (w_out_o0, w_out_o1), att_s, (att_b0, att_b1), *weights, part)
        recv = swap_c(sib_part)
        att_o = attend(after(sc(tp), sib_part), q, k, vt, SHARD, 0, 6)
        out = out_rows(vec1(own * 2), SHARD, m_oth, (w_out_o0, w_out_o1), att_o, (att_b0, att_b1), *weights, part,
                  (recv, x, gate, b_out[None]))
        return out[None]

    in_specs = (P('dp', 'tp', None), P('dp', None), P('dp'), P('dp', None), P(None, None), P(None), P(None, None, 'tp'), P(None, 'tp'), P(None), P(None), P(None, 'tp'), P('tp'), P('tp', None), P('tp', None), P(None))
    return jax.shard_map(local_step, mesh=mesh, in_specs=in_specs, out_specs=P('dp', 'tp', None), check_vma=False)
```

```python
import functools
import jax
import jax.numpy as jnp
import numpy as np
from jax import lax
from jax.experimental import pallas as pl
from jax.experimental.pallas import tpu as pltpu
from jax.sharding import PartitionSpec as P


SEQ = 6144
D = 3072
HD = 128
TXT = 256
VID = SEQ - TXT
EPS = 1e-6
THETA = 256.0
SHARD = 1536
CHIP = 2 * SHARD
DQ = 768
NH = DQ // HD
LOG2E = 1.4426950408889634
BF = jnp.bfloat16
F32 = jnp.float32
NT = (((1,), (1,)), ((), ()))
X_PAIRS = [(0, 2), (1, 3), (2, 0), (3, 1)]
C_PAIRS = [(0, 1), (1, 0), (2, 3), (3, 2)]


def params(mib=60, **kw):
    return pltpu.CompilerParams(vmem_limit_bytes=mib * 2 ** 20, **kw)


def cost(flops, nbytes):
    return pl.CostEstimate(flops=int(flops), bytes_accessed=int(nbytes), transcendentals=0)


PS = 12
MB = 3 * D // PS
RB = SEQ // PS
NB = SHARD // PS
YB = 256
FREQ = np.zeros((1, HD), np.float32)
for _l in range(HD):
    _p = _l // 2
    _d, _w = (16.0, _p) if _p < 8 else (56.0, _p - 8) if _p < 36 else (56.0, _p - 36)
    FREQ[0, _l] = np.float32(THETA) ** np.float32(-2.0 * _w / _d)


def prep_kernel(grid_ref, c_ref, wm_ref, bm_ref, x_ref, f_ref, qg_ref, kg_ref,
                y_ref, cos_ref, sin_ref, gate_ref, lim_ref, q_ref, k_ref, vt_ref, act_ref, mod_ref, nrm_ref):
    p = pl.program_id(0)

    @pl.when(p == 0)
    def _():
        c = c_ref[...]
        a = (c * jax.nn.sigmoid(c)).astype(BF)
        act_ref[...] = jnp.broadcast_to(a, (16, D))
        even = lax.broadcasted_iota(jnp.int32, (8, HD), 1) % 2 == 0

        def pair(g_ref):
            g = jnp.broadcast_to(jnp.abs(g_ref[...]), (8, HD))
            return jnp.maximum(g, jnp.where(even, pltpu.roll(g, HD - 1, 1), pltpu.roll(g, 1, 1)))

        bound = pair(qg_ref) * pair(kg_ref) * (HD ** 0.5 * LOG2E)
        lim_ref[...] = jnp.where(bound <= 96.0, 0.0, 1e30)

    @pl.when(p < PS)
    def _():
        m = jnp.dot(act_ref[...], wm_ref[...], preferred_element_type=F32)
        mod_ref[pl.ds(p, 1)] = (m[0:1] + bm_ref[...])[None]
        row = p * RB + lax.broadcasted_iota(jnp.int32, (RB, HD), 0)
        lane = lax.broadcasted_iota(jnp.int32, (1, HD), 1)
        n = row.astype(F32)
        gh = jnp.full((1, HD), grid_ref[0], jnp.int32).astype(F32)
        gw = jnp.full((1, HD), grid_ref[1], jnp.int32).astype(F32)
        line = jnp.floor((n + 0.5) * (1.0 / gw))
        frame = jnp.floor((line + 0.5) * (1.0 / gh))
        pos = jnp.where(lane < 16, frame, jnp.where(lane < 72, line - frame * gh, n - line * gw))
        ang = jnp.where(row < VID, pos * f_ref[...], 0.0)
        turn = jnp.floor(ang * 0.6366197723675814 + 0.5)
        r = ((ang - turn * 1.5703125) - turn * 4.837512969970703e-4) - turn * 7.549789954891882e-8
        z = r * r
        s = r + r * z * (-1.6666654611e-1 + z * (8.3321608736e-3 - z * 1.9515295891e-4))
        c = 1.0 - 0.5 * z + z * z * (4.166664568298827e-2 + z * (-1.388731625493765e-3 + z * 2.443315711809948e-5))
        t = turn.astype(jnp.int32)
        odd = (t & 1) == 1
        sv = jnp.where(odd, c, s)
        cv = jnp.where(odd, s, c)
        cos_ref[...] = jnp.where(((t + 1) & 2) == 2, -cv, cv)
        sin_ref[...] = jnp.where(((t & 2) == 2) != (lane % 2 == 0), -sv, sv)
        x = x_ref[...].astype(F32)
        d = x - jnp.mean(x, axis=-1, keepdims=True)
        var = jnp.mean(d * d, axis=-1, keepdims=True)
        nrm_ref[pl.ds(pl.multiple_of(p * NB, NB), NB), :] = d * lax.rsqrt(var + EPS)

    @pl.when(p == PS)
    def _():
        for j in range(PS // 3):
            gate_ref[0:1, pl.ds(j * MB, MB)] = mod_ref[2 * PS // 3 + j]

    @pl.when(p >= PS)
    def _():
        at = pl.multiple_of((p - PS) * YB, YB)
        for j in range(PS // 3):
            col = pl.ds(j * MB, MB)
            y_ref[:, col] = (nrm_ref[pl.ds(at, YB), col] * (1.0 + mod_ref[PS // 3 + j]) + mod_ref[j]).astype(BF)


def prep(grid_hw, cond, w_mod, b_mod, x, qg, kg):
    lo = lambda p: jnp.minimum(p, PS - 1)
    full = lambda *s: pl.BlockSpec(s, lambda p, g: (0,) * len(s))
    anyspec = pl.BlockSpec(memory_space=pl.ANY)
    return pl.pallas_call(
        prep_kernel,
        grid_spec=pltpu.PrefetchScalarGridSpec(
            num_scalar_prefetch=1, grid=(PS + SHARD // YB,),
            in_specs=[full(1, D), pl.BlockSpec((D, MB), lambda p, g: (0, lo(p))), pl.BlockSpec((1, MB), lambda p, g: (0, lo(p))),
                      pl.BlockSpec((NB, D), lambda p, g: (lo(p), 0)), full(1, HD), full(1, HD), full(1, HD)],
            out_specs=[pl.BlockSpec((YB, D), lambda p, g: (jnp.maximum(p - PS, 0), 0)),
                       pl.BlockSpec((RB, HD), lambda p, g: (lo(p), 0)), pl.BlockSpec((RB, HD), lambda p, g: (lo(p), 0)),
                       full(1, D), full(8, HD), anyspec, anyspec, anyspec],
            scratch_shapes=[pltpu.VMEM((16, D), BF), pltpu.VMEM((PS, 1, MB), F32), pltpu.VMEM((SHARD, D), F32)]),
        out_shape=[jax.ShapeDtypeStruct((SHARD, D), BF), jax.ShapeDtypeStruct((SEQ, HD), F32), jax.ShapeDtypeStruct((SEQ, HD), F32),
                   jax.ShapeDtypeStruct((1, D), F32), jax.ShapeDtypeStruct((8, HD), F32),
                   jax.ShapeDtypeStruct((SEQ, DQ), BF), jax.ShapeDtypeStruct((SEQ, DQ), BF), jax.ShapeDtypeStruct((DQ, SEQ), BF)],
        compiler_params=params(), cost_estimate=cost(2e10, 9e7), name="prep")(
            grid_hw.reshape(2), cond, w_mod, b_mod[None], x, FREQ, qg, kg)


QBM = 512
SUB = 256


def qkv_kernel(which_ref, sc_ref, y_ref, w_ref, b_ref, qg_ref, kg_ref, cos_ref, sin_ref, lim_in, _q, _k, _v,
               q_ref, k_ref, vt_ref, lim_ref, left0, left1):
    n = pl.program_id(1)
    tiles = [(i, s) for i in range(QBM // SUB) for s in range(DQ // SUB)]
    pairs = [tiles[a:a + 2] for a in range(0, len(tiles), 2)]

    @pl.when(jnp.logical_and(pl.program_id(0) == 0, n == 0))
    def _():
        lim_ref[...] = lim_in[...]

    def proj(t):
        return jnp.dot(y_ref[pl.ds(t[0] * SUB, SUB), :], w_ref[0, :, pl.ds(t[1] * SUB, SUB)], preferred_element_type=F32)

    def rope(r, t, gain, row, out_ref):
        at = pl.ds(t[0] * SUB, SUB)
        even = lax.broadcasted_iota(jnp.int32, (SUB, HD), 1) % 2 == 0
        for h in range(SUB // HD):
            lo = t[1] * SUB + h * HD
            x = r[:, h * HD:(h + 1) * HD] + b_ref[row:row + 1, lo:lo + HD]
            ms = jnp.mean(x * x, axis=-1, keepdims=True)
            x = x * lax.rsqrt(ms + EPS) * gain
            partner = jnp.where(even, pltpu.roll(x, HD - 1, 1), pltpu.roll(x, 1, 1))
            out_ref[at, lo:lo + HD] = (x * cos_ref[at, :] + partner * sin_ref[at, :]).astype(BF)

    def put(r, t):
        lo = t[1] * SUB
        v = r + b_ref[2:3, lo:lo + SUB]
        vt_ref[pl.ds(lo, SUB), pl.ds(t[0] * SUB, SUB)] = v.T.astype(BF)
        top = jnp.max(jnp.abs(v).reshape(SUB // 8, 8, SUB), axis=0)
        lim_ref[...] = jnp.maximum(lim_ref[...], jnp.maximum(top[:, :HD], top[:, HD:]))

    def q_epi(r, t):
        rope(r, t, qg_ref[...] * (LOG2E * HD ** -0.5), 0, q_ref)

    def k_epi(r, t):
        rope(r, t, kg_ref[...], 1, k_ref)

    def run(epi, before, keep):
        held = []
        for p, pair in enumerate(pairs):
            last = keep and p == len(pairs) - 1
            now = [(proj(t), t) for t in pair]
            if last:
                left0[...] = now[0][0]
                left1[...] = now[1][0]
            if p == 0 and before is not None:
                before(left0[...], pairs[-1][0])
                before(left1[...], pairs[-1][1])
            for r, t in held:
                epi(r, t)
            held = [] if last else now
        for r, t in held:
            epi(r, t)

    @pl.when(n == 0)
    def _():
        run(q_epi, None, True)

    @pl.when(n == 1)
    def _():
        run(k_epi, q_epi, True)

    @pl.when(n == 2)
    def _():
        run(put, k_epi, False)


def qkv(which, sc, y, w3, b, qg, kg, cos, sin, lim, bufs):
    m = SHARD // QBM
    at = lambda i, w, s: s[w[0]] * m + i
    full = lambda *s: pl.BlockSpec(s, lambda i, n, w, s_: (0,) * len(s))
    anyspec = pl.BlockSpec(memory_space=pl.ANY)
    return pl.pallas_call(
        qkv_kernel,
        grid_spec=pltpu.PrefetchScalarGridSpec(
            num_scalar_prefetch=2, grid=(m, 3),
            in_specs=[pl.BlockSpec((QBM, D), lambda i, n, w, s: (i, 0)),
                      pl.BlockSpec((1, D, DQ), lambda i, n, w, s: (n, 0, 0)),
                      full(3, DQ), full(1, HD), full(1, HD),
                      pl.BlockSpec((QBM, HD), lambda i, n, w, s: (at(i, w, s), 0)),
                      pl.BlockSpec((QBM, HD), lambda i, n, w, s: (at(i, w, s), 0)),
                      full(8, HD), anyspec, anyspec, anyspec],
            out_specs=[pl.BlockSpec((QBM, DQ), lambda i, n, w, s: (at(i, w, s), 0)),
                       pl.BlockSpec((QBM, DQ), lambda i, n, w, s: (at(i, w, s), 0)),
                       pl.BlockSpec((DQ, QBM), lambda i, n, w, s: (0, at(i, w, s))),
                       full(8, HD)],
            scratch_shapes=[pltpu.VMEM((SUB, SUB), F32)] * 2),
        out_shape=[jax.ShapeDtypeStruct((SEQ, DQ), BF), jax.ShapeDtypeStruct((SEQ, DQ), BF),
                   jax.ShapeDtypeStruct((DQ, SEQ), BF), jax.ShapeDtypeStruct((8, HD), F32)],
        input_output_aliases={10: 0, 11: 1, 12: 2}, compiler_params=params(),
        cost_estimate=cost(2 * SHARD * D * 3 * DQ, SHARD * D * 2 + 3 * D * DQ * 2), name="qkv")(
            which, sc, y, w3, b, qg, kg, cos, sin, lim, *bufs)


BQ = SHARD
BK = 512


def attn_kernel(head_ref, which_ref, row_ref, sc_ref, lim_ref, q_ref, k_ref, vt_ref, *refs):
    o_ref, flag_ref = refs[-2:]
    txt_len = sc_ref[4]

    @pl.when(pl.program_id(0) == 0)
    def _():
        flag_ref[0] = (jnp.max(lim_ref[...]) <= 4096.0).astype(jnp.int32)

    bq = q_ref.shape[0]
    nk = SEQ // BK
    last = BK - TXT
    first_row = sc_ref[which_ref[pl.program_id(0)]] * bq
    has_pad = jnp.logical_and(first_row + bq == SEQ, txt_len < TXT)

    def scores(j):
        return lax.dot_general(k_ref[pl.ds(j * BK, BK), :], q_ref[...], NT, preferred_element_type=F32)

    def key_ok():
        return lax.broadcasted_iota(jnp.int32, (BK, 1), 0) < last + txt_len

    def finish(acc, l):
        o = acc * (1.0 / l)
        o_ref[...] = o.T.astype(BF)

        @pl.when(has_pad)
        def _():
            s = lax.dot_general(k_ref[pl.ds(VID, TXT), :], q_ref[...], NT, preferred_element_type=F32)
            pad_key = lax.broadcasted_iota(jnp.int32, (TXT, 1), 0) >= txt_len
            s = jnp.where(pad_key, s, -1e30)
            p = jnp.exp2(s - jnp.max(s, axis=0, keepdims=True))
            lp = jnp.sum(p, axis=0, keepdims=True)
            ap = jnp.dot(vt_ref[:, pl.ds(VID, TXT)], p.astype(BF), preferred_element_type=F32)
            row = first_row + lax.broadcasted_iota(jnp.int32, (bq, 1), 0)
            o_ref[...] = jnp.where(row < VID + txt_len, o_ref[...].astype(F32), (ap * (1.0 / lp)).T).astype(BF)

    @pl.when(flag_ref[0] == 1)
    def _():
        acc = jnp.zeros((HD, bq), F32)
        l = jnp.zeros((1, bq), F32)
        s = scores(0)
        for j in range(nk):
            nxt = scores(j + 1) if j + 1 < nk else None
            p = jnp.exp2(s)
            if j == nk - 1:
                p = jnp.where(key_ok(), p, 0.0)
            l = l + jnp.sum(p, axis=0, keepdims=True)
            acc = acc + jnp.dot(vt_ref[:, pl.ds(j * BK, BK)], p.astype(BF), preferred_element_type=F32)
            s = nxt
        finish(acc, l)

    @pl.when(flag_ref[0] == 0)
    def _():
        def step(j, carry):
            m, l, acc = carry
            at = pl.multiple_of(j * BK, BK)
            s = lax.dot_general(k_ref[pl.ds(at, BK), :], q_ref[...], NT, preferred_element_type=F32)
            s = jnp.where(jnp.logical_or(key_ok(), j < nk - 1), s, -1e30)
            mn = jnp.maximum(m, jnp.max(s, axis=0, keepdims=True))
            p = jnp.exp2(s - mn)
            a = jnp.exp2(m - mn)
            l = l * a + jnp.sum(p, axis=0, keepdims=True)
            acc = acc * a + jnp.dot(vt_ref[:, pl.ds(at, BK)], p.astype(BF), preferred_element_type=F32)
            return mn, l, acc

        init = (jnp.full((1, bq), -1e30, F32), jnp.zeros((1, bq), F32), jnp.zeros((HD, bq), F32))
        _, l, acc = lax.fori_loop(0, nk, step, init)
        finish(acc, l)


def attend(pairs, blocks, sc, lim, q, k, vt, into=None):
    n = len(pairs)
    head, which, row = (np.array(v, np.int32) for v in zip(*(pairs + [pairs[-1]] * (16 - n))))
    in_specs = [pl.BlockSpec((8, HD), lambda i, h, w, r, s: (0, 0)),
                pl.BlockSpec((BQ, HD), lambda i, h, w, r, s: (s[w[i]], h[i])),
                pl.BlockSpec((SEQ, HD), lambda i, h, w, r, s: (0, h[i])),
                pl.BlockSpec((HD, SEQ), lambda i, h, w, r, s: (h[i], 0))]
    args = [head, which, row, sc, lim, q, k, vt]
    if into is not None:
        in_specs.append(pl.BlockSpec(memory_space=pl.ANY))
        args.append(into)
    return pl.pallas_call(
        attn_kernel,
        grid_spec=pltpu.PrefetchScalarGridSpec(
            num_scalar_prefetch=4, grid=(n,), in_specs=in_specs,
            out_specs=pl.BlockSpec((BQ, HD), lambda i, h, w, r, s: (r[i], h[i])),
            scratch_shapes=[pltpu.SMEM((1,), jnp.int32)]),
        out_shape=jax.ShapeDtypeStruct((blocks * BQ, DQ), BF), input_output_aliases={} if into is None else {8: 0},
        compiler_params=params(), cost_estimate=cost(6 * n * BQ * SEQ * HD, 4 * HD * n * (SEQ + BQ)), name="attend")(*args)


KC = 512
BN = 512
NL = BN // HD
NK = D // KC
NX = D // HD
NJ = D // BN
TILES = tuple((r, 256) for r in range(0, SHARD, 256))


def gelu(u):
    h = 0.5 * u
    t = jnp.tanh(u * (0.7978845608028654 + 0.03567740813636141 * (u * u)))
    return (h * t + h).astype(BF)


def dot(a, b):
    return jnp.dot(jnp.concatenate(a, axis=1), jnp.concatenate(b, axis=1), preferred_element_type=F32)


def tiled(product, store):
    held = None
    for tile in TILES:
        now = product(tile)
        if held is not None:
            store(*held)
        held = (tile, now)
    store(*held)


def started(copies):
    for c in copies:
        c.start()


def waited(copies):
    for c in copies:
        c.wait()


def mlp_kernel(fused, y0_ref, y1_ref, wa_ref, wb_ref, b_ref, o_ref, xs, ws, sx, sw, sf, *more):
    i = pl.program_id(0)
    s = pl.program_id(1)
    steps = 2 * NJ if fused else NJ
    slot = (i * steps + s) % 2

    def copy_x(y_ref, at, c):
        return [pltpu.make_async_copy(y_ref.at[:, pl.ds(x * HD, HD)], xs.at[at, x], sx.at[at, x]) for x in range(c * NL, c * NL + NL)]

    def columns(col, n):
        return pl.ds(pl.multiple_of(col * BN + n * HD, HD), HD)

    def copy_w(w_ref, col, at):
        return [pltpu.make_async_copy(w_ref.at[:, columns(col, n)], ws.at[at, n], sw.at[at, n]) for n in range(NL)]

    def first_w(c):
        k = pl.ds(c * KC, KC)
        return [pltpu.make_async_copy(wa_ref.at[k, columns(0, n)], ws.at[0, n, k], sf.at[c, n]) for n in range(NL)]

    first = jnp.logical_and(i == 0, s == 0)
    half = wa_ref.shape[1] // BN

    @pl.when(first)
    def _():
        for c in range(NK):
            started(copy_x(y0_ref, 0, c))
            started(first_w(c))

    @pl.when(s + 1 < half)
    def _():
        started(copy_w(wa_ref, s + 1, 1 - slot))

    @pl.when(jnp.logical_and(s + 1 >= half, s + 1 < steps))
    def _():
        started(copy_w(wb_ref, s + 1 - half, 1 - slot))

    @pl.when(jnp.logical_and(s + 1 == steps, i == 0))
    def _():
        started(copy_w(wa_ref, 0, 1 - slot))

    @pl.when(jnp.logical_and(s == 1, i == 0))
    def _():
        for c in range(NK):
            started(copy_x(y1_ref, 1, c))

    @pl.when(jnp.logical_and(s == 0, i == 1))
    def _():
        for c in range(NK):
            waited(copy_x(y1_ref, 1, c))

    bias = b_ref[:, pl.ds(pl.multiple_of(jnp.minimum(s, NJ - 1) * BN, BN), BN)]

    def put(tile, u):
        g = gelu(u + bias)
        if fused:
            for n in range(NL):
                more[0][s * NL + n, pl.ds(*tile), :] = g[:, n * HD:(n + 1) * HD]
        else:
            o_ref[pl.ds(*tile), :] = g

    @pl.when(first)
    def _():
        acc = [None] * len(TILES)
        for c in range(NK):
            waited(copy_x(y0_ref, 0, c))
            waited(first_w(c))
            w = [ws[0, n, pl.ds(c * KC, KC), :] for n in range(NL)]
            for n, tile in enumerate(TILES):
                r = dot([xs[0, x, pl.ds(*tile), :] for x in range(c * NL, c * NL + NL)], w)
                acc[n] = r if c == 0 else acc[n] + r
        for tile, u in zip(TILES, acc):
            put(tile, u)

    @pl.when(jnp.logical_not(first))
    def _():
        waited(copy_w(wa_ref, 0, slot))

    def weights():
        return [ws[slot, n] for n in range(NL)]

    @pl.when(jnp.logical_and(jnp.logical_not(first), s < NJ))
    def _():
        tiled(lambda tile: dot([xs[i, x, pl.ds(*tile), :] for x in range(NX)], weights()), put)

    if fused:
        @pl.when(s >= NJ)
        def _():
            def store(tile, r):
                o_ref[pl.ds(*tile), :] = r

            tiled(lambda tile: dot([more[0][x, pl.ds(*tile), :] for x in range(NX)], weights()), store)


def mlp(fused, y0, y1, wa, wb, b):
    steps = 2 * NJ if fused else NJ
    anyspec = pl.BlockSpec(memory_space=pl.ANY)
    dma = pltpu.SemaphoreType.DMA
    if fused:
        omap = lambda i, s: (jnp.where(s >= NJ, i, 0), jnp.where(s >= NJ, s - NJ, jnp.where(i == 0, 0, NJ - 1)))
    else:
        omap = lambda i, s: (i, s)
    scratch = [pltpu.VMEM((2, NX, SHARD, HD), BF), pltpu.VMEM((2, NL, D, HD), BF), dma((2, NX)), dma((2, NL)), dma((NK, NL))]
    return pl.pallas_call(
        functools.partial(mlp_kernel, fused), grid=(2, steps),
        in_specs=[anyspec] * 4 + [pl.BlockSpec((1, D), lambda i, s: (0, 0))],
        out_specs=pl.BlockSpec((SHARD, BN), omap), out_shape=jax.ShapeDtypeStruct((CHIP, D), F32 if fused else BF),
        scratch_shapes=scratch + ([pltpu.VMEM((NX, SHARD, HD), BF)] if fused else []),
        compiler_params=params(), cost_estimate=cost(2 * CHIP * D * steps * BN, CHIP * D * 8), name="mlp")(y0, y1, wa, wb, b)


KO = D + 2 * DQ
NP = 3
OCHUNKS = tuple((c * KC, KC) for c in range(NK)) + ((D, DQ), (D + DQ, DQ))


def out_kernel(final, first_row, a0_row, *refs):
    m_ref, *w_refs, a0_ref, a1_ref, v0_ref, v1_ref, p_ref = refs[:6 + NP]
    extra = refs[6 + NP:10 + NP] if final else ()
    o_ref, xs, ws, ps, sx, sw, sp = refs[6 + NP + len(extra):6 + NP + len(extra) + 7]
    j = pl.program_id(0)
    slot = j % 2
    if final:
        recv_ref, t_ref, gate_ref, bo_ref = extra
        rs, ts, sr, st = refs[-4:]

    def copy_x(c):
        k, n = OCHUNKS[c]
        cs = []
        for x in range(k // HD, (k + n) // HD):
            if k < D:
                s = m_ref.at[pl.ds(first_row, SHARD), pl.ds(x * HD, HD)]
            else:
                a_ref, row = (a0_ref, a0_row) if k == D else (a1_ref, 0)
                s = a_ref.at[pl.ds(row, SHARD), pl.ds(x * HD - k, HD)]
            cs.append(pltpu.make_async_copy(s, xs.at[x], sx.at[x]))
        return cs

    def copy_w(c, col, at):
        k, n = OCHUNKS[c]
        piece = D // NP
        w_ref, top = (w_refs[k // piece], k % piece) if k < D else (v0_ref, 0) if k == D else (v1_ref, 0)
        cols = lambda l: pl.ds(pl.multiple_of(col * BN + l * HD, HD), HD)
        return [pltpu.make_async_copy(w_ref.at[pl.ds(top, n), cols(l)], ws.at[at, l, pl.ds(k, n)], sw.at[at, c, l]) for l in range(NL)]

    def copy_tail(col, at):
        col = pl.ds(pl.multiple_of(col * BN, BN), BN)
        cs = [pltpu.make_async_copy(p_ref.at[pl.ds(first_row, SHARD), col], ps.at[at], sp.at[at])]
        if final:
            cs += [pltpu.make_async_copy(recv_ref.at[:, col], rs.at[at], sr.at[at]), pltpu.make_async_copy(t_ref.at[:, col], ts.at[at], st.at[at])]
        return cs

    chunks = range(len(OCHUNKS))

    @pl.when(j == 0)
    def _():
        for c in chunks:
            started(copy_x(c))
            started(copy_w(c, 0, 0))
        started(copy_tail(0, 0))

    @pl.when(j + 1 < NJ)
    def _():
        for c in chunks:
            started(copy_w(c, j + 1, 1 - slot))
        started(copy_tail(j + 1, 1 - slot))

    def store(tile, acc):
        rows = pl.ds(*tile)
        acc = acc + ps[slot, rows, :]
        if final:
            acc = ts[slot, rows, :].astype(F32) + gate_ref[...] * (acc + rs[slot, rows, :] + bo_ref[...])
        o_ref[rows, :] = acc.astype(o_ref.dtype)

    @pl.when(j == 0)
    def _():
        acc = [None] * len(TILES)
        for c in chunks:
            waited(copy_x(c))
            waited(copy_w(c, 0, 0))
            k, n = OCHUNKS[c]
            w = [ws[0, l, pl.ds(k, n), :] for l in range(NL)]
            for a, tile in enumerate(TILES):
                r = dot([xs[x, pl.ds(*tile), :] for x in range(k // HD, (k + n) // HD)], w)
                acc[a] = r if c == 0 else acc[a] + r
        waited(copy_tail(0, 0))
        for tile, r in zip(TILES, acc):
            store(tile, r)

    @pl.when(j > 0)
    def _():
        for c in chunks:
            waited(copy_w(c, 0, slot))
        waited(copy_tail(0, slot))
        tiled(lambda tile: dot([xs[x, pl.ds(*tile), :] for x in range(KO // HD)], [ws[slot, l] for l in range(NL)]), store)


def out_rows(first_row, a0_row, m, wms, a0, a1, v0, v1, part, tail=None):
    anyspec = pl.BlockSpec(memory_space=pl.ANY)
    vec = pl.BlockSpec((1, BN), lambda j: (0, j))
    final = tail is not None
    nc = len(OCHUNKS)
    dma = pltpu.SemaphoreType.DMA
    scratch = [pltpu.VMEM((KO // HD, SHARD, HD), BF), pltpu.VMEM((2, NL, KO, HD), BF), pltpu.VMEM((2, SHARD, BN), F32),
               dma((KO // HD,)), dma((2, nc, NL)), dma((2,))]
    if final:
        scratch += [pltpu.VMEM((2, SHARD, BN), F32), pltpu.VMEM((2, SHARD, BN), BF), dma((2,)), dma((2,))]
    return pl.pallas_call(
        functools.partial(out_kernel, final, first_row, a0_row), grid=(NJ,),
        in_specs=[anyspec] * (6 + NP) + ([anyspec, anyspec, vec, vec] if final else []),
        out_specs=pl.BlockSpec((SHARD, BN), lambda j: (0, j)),
        out_shape=jax.ShapeDtypeStruct((SHARD, D), BF if final else F32), scratch_shapes=scratch, compiler_params=params(),
        cost_estimate=cost(2 * SHARD * KO * D, SHARD * D * 14), name="out_rows")(m, *wms, a0, a1, v0, v1, part, *(tail or ()))


def after(v, *deps):
    return lax.optimization_barrier((v,) + deps)[0]


def solution(mesh):
    def local_step(tokens, cond_vec, txt_len, grid_hw, w_mod, b_mod, w_qkv, b_qkv, q_gain, k_gain,
                   w_mlp_in, b_mlp_in, w_out_attn, w_out_mlp, b_out):
        tp = lax.axis_index('tp')
        dp = lax.axis_index('dp')
        own = tp % 2
        x = tokens[0]

        def swap_x(v):
            return lax.ppermute(v, 'tp', X_PAIRS)

        def swap_c(v):
            return lax.ppermute(v, 'tp', C_PAIRS)

        gather = lambda v: lax.all_gather(v, 'dp', axis=0, tiled=True)

        q4 = D // 4
        split = D // 3
        hop_in = [swap_x(lax.dynamic_slice(w_mlp_in, (dp * q4, lo), (q4, n)))
                  for lo, n in ((0, split), (split, D - split))]
        hop_att = swap_x(lax.dynamic_slice_in_dim(w_out_attn, dp * (DQ // 4), DQ // 4, 0))
        hop_out = [swap_x(lax.dynamic_slice_in_dim(w_out_mlp, c * split + dp * (split // 4), split // 4, 0)) for c in range(NP)]
        b_in_o = swap_x(b_mlp_in)[None]

        sib = tp + 1 - 2 * own
        rem = (tp + 2) % 4
        remsib = (sib + 2) % 4
        sc = jnp.stack([tp, sib, rem, remsib, txt_len[0]]).astype(jnp.int32)
        OWN, SIB, REM, REMSIB = (np.full((1,), i, np.int32) for i in range(4))

        qg = q_gain[None]
        kg = k_gain[None]
        y, cos, sin, gate, lim, *bufs = prep(grid_hw, cond_vec, w_mod, b_mod, x, qg, kg)
        y_sib = swap_c(y)
        y_rem = swap_x(y)
        tabs = (jnp.transpose(w_qkv, (1, 0, 2)), b_qkv, qg, kg, cos, sin)

        w_in_o0 = gather(after(hop_in[0], y))
        *bufs, lim = qkv(OWN, sc, y, *tabs, lim, bufs)
        *bufs, lim = qkv(SIB, sc, y_sib, *tabs, lim, bufs)
        w_in_o1 = gather(after(hop_in[1], lim))
        part = mlp(True, y, after(y_sib, lim), w_mlp_in, w_out_mlp, b_mlp_in[None])
        w_att_o = gather(after(hop_att, part))
        m_oth = mlp(False, y, y_sib, w_in_o0, w_in_o1, b_in_o)
        y_rem = after(y_rem, m_oth)
        y_remsib = swap_c(y_rem)
        *bufs, lim = qkv(REM, sc, y_rem, *tabs, lim, bufs)
        w_out_o = [gather(after(hop_out[0], lim))]
        q, k, vt, lim = qkv(REMSIB, sc, y_remsib, *tabs, lim, bufs)
        w_out_o.append(gather(after(hop_out[1], lim)))

        att_r0 = attend([(h, 3, 0) for h in range(NH)], 1, sc, lim, q, k, vt)
        att_b0 = swap_x(att_r0)
        w_out_o.append(gather(after(hop_out[2], att_r0)))
        att_r1 = attend([(h, 2, 0) for h in range(NH)], 1, after(sc, att_r0), lim, q, k, vt)
        att_b1 = swap_x(att_r1)
        some = NH // 2
        att_a = attend([(h, 1, 0) for h in range(NH)] + [(h, 0, 1) for h in range(some)], 2, after(sc, att_r1), lim, q, k, vt)

        wms = tuple(w_out_o)
        weights = (w_out_attn, w_att_o, part)
        sib_part = out_rows(SHARD, 0, m_oth, wms, att_a, att_b0, *weights)
        recv = swap_c(sib_part)
        att_a = attend([(h, 0, 1) for h in range(some, NH)], 2, after(sc, sib_part), lim, q, k, vt, after(att_a, sib_part))
        out = out_rows(0, SHARD, m_oth, wms, att_a, att_b1, *weights, (recv, x, gate, b_out[None]))
        return out[None]

    in_specs = (P('dp', 'tp', None), P('dp', None), P('dp'), P('dp', None), P(None, None), P(None), P(None, None, 'tp'), P(None, 'tp'), P(None), P(None), P(None, 'tp'), P('tp'), P('tp', None), P('tp', None), P(None))
    return jax.shard_map(local_step, mesh=mesh, in_specs=in_specs, out_specs=P('dp', 'tp', None), check_vma=False)
```

```python
import functools
import jax
import jax.numpy as jnp
import numpy as np
from jax import lax
from jax.experimental import pallas as pl
from jax.experimental.pallas import tpu as pltpu
from jax.sharding import PartitionSpec as P


SEQ = 6144
D = 3072
HD = 128
TXT = 256
VID = SEQ - TXT
EPS = 1e-6
THETA = 256.0
SHARD = 1536
CHIP = 2 * SHARD
DQ = 768
NH = DQ // HD
LOG2E = 1.4426950408889634
BF = jnp.bfloat16
F32 = jnp.float32
NT = (((1,), (1,)), ((), ()))
X_PAIRS = [(0, 2), (1, 3), (2, 0), (3, 1)]
C_PAIRS = [(0, 1), (1, 0), (2, 3), (3, 2)]


def params(mib=63, **kw):
    return pltpu.CompilerParams(vmem_limit_bytes=mib * 2 ** 20, **kw)


def cost(flops, nbytes):
    return pl.CostEstimate(flops=int(flops), bytes_accessed=int(nbytes), transcendentals=0)


PS = 12
MB = 3 * D // PS
RB = SEQ // PS
NB = SHARD // PS
YB = 256
FREQ = np.zeros((1, HD), np.float32)
for _l in range(HD):
    _p = _l // 2
    _d, _w = (16.0, _p) if _p < 8 else (56.0, _p - 8) if _p < 36 else (56.0, _p - 36)
    FREQ[0, _l] = np.float32(THETA) ** np.float32(-2.0 * _w / _d)


def prep_kernel(grid_ref, c_ref, wm_ref, bm_ref, x_ref, f_ref, qg_ref, kg_ref,
                y_ref, cos_ref, sin_ref, gate_ref, lim_ref, q_ref, k_ref, vt_ref, act_ref, mod_ref, nrm_ref):
    p = pl.program_id(0)

    @pl.when(p == 0)
    def _():
        c = c_ref[...]
        a = (c * jax.nn.sigmoid(c)).astype(BF)
        act_ref[...] = jnp.broadcast_to(a, (16, D))
        even = lax.broadcasted_iota(jnp.int32, (8, HD), 1) % 2 == 0

        def pair(g_ref):
            g = jnp.broadcast_to(jnp.abs(g_ref[...]), (8, HD))
            return jnp.maximum(g, jnp.where(even, pltpu.roll(g, HD - 1, 1), pltpu.roll(g, 1, 1)))

        bound = pair(qg_ref) * pair(kg_ref) * (HD ** 0.5 * LOG2E)
        lim_ref[...] = jnp.where(bound <= 96.0, 0.0, 1e30)

    @pl.when(p < PS)
    def _():
        m = jnp.dot(act_ref[...], wm_ref[...], preferred_element_type=F32)
        mod_ref[pl.ds(p, 1)] = (m[0:1] + bm_ref[...])[None]
        row = p * RB + lax.broadcasted_iota(jnp.int32, (RB, HD), 0)
        lane = lax.broadcasted_iota(jnp.int32, (1, HD), 1)
        n = row.astype(F32)
        gh = jnp.full((1, HD), grid_ref[0], jnp.int32).astype(F32)
        gw = jnp.full((1, HD), grid_ref[1], jnp.int32).astype(F32)
        line = jnp.floor((n + 0.5) * (1.0 / gw))
        frame = jnp.floor((line + 0.5) * (1.0 / gh))
        pos = jnp.where(lane < 16, frame, jnp.where(lane < 72, line - frame * gh, n - line * gw))
        ang = jnp.where(row < VID, pos * f_ref[...], 0.0)
        turn = jnp.floor(ang * 0.6366197723675814 + 0.5)
        r = ((ang - turn * 1.5703125) - turn * 4.837512969970703e-4) - turn * 7.549789954891882e-8
        z = r * r
        s = r + r * z * (-1.6666654611e-1 + z * (8.3321608736e-3 - z * 1.9515295891e-4))
        c = 1.0 - 0.5 * z + z * z * (4.166664568298827e-2 + z * (-1.388731625493765e-3 + z * 2.443315711809948e-5))
        t = turn.astype(jnp.int32)
        odd = (t & 1) == 1
        sv = jnp.where(odd, c, s)
        cv = jnp.where(odd, s, c)
        cos_ref[...] = jnp.where(((t + 1) & 2) == 2, -cv, cv)
        sin_ref[...] = jnp.where(((t & 2) == 2) != (lane % 2 == 0), -sv, sv)
        x = x_ref[...].astype(F32)
        d = x - jnp.mean(x, axis=-1, keepdims=True)
        var = jnp.mean(d * d, axis=-1, keepdims=True)
        nrm_ref[pl.ds(pl.multiple_of(p * NB, NB), NB), :] = d * lax.rsqrt(var + EPS)

    @pl.when(p == PS)
    def _():
        for j in range(PS // 3):
            gate_ref[0:1, pl.ds(j * MB, MB)] = mod_ref[2 * PS // 3 + j]

    @pl.when(p >= PS)
    def _():
        at = pl.multiple_of((p - PS) * YB, YB)
        for j in range(PS // 3):
            col = pl.ds(j * MB, MB)
            y_ref[:, col] = (nrm_ref[pl.ds(at, YB), col] * (1.0 + mod_ref[PS // 3 + j]) + mod_ref[j]).astype(BF)


def prep(grid_hw, cond, w_mod, b_mod, x, qg, kg):
    lo = lambda p: jnp.minimum(p, PS - 1)
    full = lambda *s: pl.BlockSpec(s, lambda p, g: (0,) * len(s))
    anyspec = pl.BlockSpec(memory_space=pl.ANY)
    return pl.pallas_call(
        prep_kernel,
        grid_spec=pltpu.PrefetchScalarGridSpec(
            num_scalar_prefetch=1, grid=(PS + SHARD // YB,),
            in_specs=[full(1, D), pl.BlockSpec((D, MB), lambda p, g: (0, lo(p))), pl.BlockSpec((1, MB), lambda p, g: (0, lo(p))),
                      pl.BlockSpec((NB, D), lambda p, g: (lo(p), 0)), full(1, HD), full(1, HD), full(1, HD)],
            out_specs=[pl.BlockSpec((YB, D), lambda p, g: (jnp.maximum(p - PS, 0), 0)),
                       pl.BlockSpec((RB, HD), lambda p, g: (lo(p), 0)), pl.BlockSpec((RB, HD), lambda p, g: (lo(p), 0)),
                       full(1, D), full(8, HD), anyspec, anyspec, anyspec],
            scratch_shapes=[pltpu.VMEM((16, D), BF), pltpu.VMEM((PS, 1, MB), F32), pltpu.VMEM((SHARD, D), F32)]),
        out_shape=[jax.ShapeDtypeStruct((SHARD, D), BF), jax.ShapeDtypeStruct((SEQ, HD), F32), jax.ShapeDtypeStruct((SEQ, HD), F32),
                   jax.ShapeDtypeStruct((1, D), F32), jax.ShapeDtypeStruct((8, HD), F32),
                   jax.ShapeDtypeStruct((SEQ, DQ), BF), jax.ShapeDtypeStruct((SEQ, DQ), BF), jax.ShapeDtypeStruct((DQ, SEQ), BF)],
        compiler_params=params(), cost_estimate=cost(2e10, 9e7), name="prep")(
            grid_hw.reshape(2), cond, w_mod, b_mod[None], x, FREQ, qg, kg)


QBM = 768
SUB = 256
SROW = 384


def qkv_kernel(which_ref, sc_ref, y_ref, w_ref, b_ref, qg_ref, kg_ref, cos_ref, sin_ref, lim_in, _q, _k, _v,
               q_ref, k_ref, vt_ref, lim_ref, left0, left1):
    n = pl.program_id(1)
    tiles = [(i, s) for i in range(QBM // SROW) for s in range(DQ // SUB)]
    pairs = [tiles[a:a + 2] for a in range(0, len(tiles), 2)]

    @pl.when(jnp.logical_and(pl.program_id(0) == 0, n == 0))
    def _():
        lim_ref[...] = lim_in[...]

    def proj(t):
        return jnp.dot(y_ref[pl.ds(t[0] * SROW, SROW), :], w_ref[0, :, pl.ds(t[1] * SUB, SUB)], preferred_element_type=F32)

    def rope(r, t, gain, row, out_ref):
        at = pl.ds(t[0] * SROW, SROW)
        even = lax.broadcasted_iota(jnp.int32, (SROW, HD), 1) % 2 == 0
        for h in range(SUB // HD):
            lo = t[1] * SUB + h * HD
            x = r[:, h * HD:(h + 1) * HD] + b_ref[row:row + 1, lo:lo + HD]
            ms = jnp.mean(x * x, axis=-1, keepdims=True)
            x = x * lax.rsqrt(ms + EPS) * gain
            partner = jnp.where(even, pltpu.roll(x, HD - 1, 1), pltpu.roll(x, 1, 1))
            out_ref[at, lo:lo + HD] = (x * cos_ref[at, :] + partner * sin_ref[at, :]).astype(BF)

    def put(r, t):
        lo = t[1] * SUB
        v = r + b_ref[2:3, lo:lo + SUB]
        vt_ref[pl.ds(lo, SUB), pl.ds(t[0] * SROW, SROW)] = v.T.astype(BF)
        top = jnp.max(jnp.abs(v).reshape(SROW // 8, 8, SUB), axis=0)
        lim_ref[...] = jnp.maximum(lim_ref[...], jnp.maximum(top[:, :HD], top[:, HD:]))

    def q_epi(r, t):
        rope(r, t, qg_ref[...] * (LOG2E * HD ** -0.5), 0, q_ref)

    def k_epi(r, t):
        rope(r, t, kg_ref[...], 1, k_ref)

    def run(epi, before, keep):
        held = []
        for p, pair in enumerate(pairs):
            last = keep and p == len(pairs) - 1
            now = [(proj(t), t) for t in pair]
            if last:
                left0[...] = now[0][0]
                left1[...] = now[1][0]
            if p == 0 and before is not None:
                before(left0[...], pairs[-1][0])
                before(left1[...], pairs[-1][1])
            for r, t in held:
                epi(r, t)
            held = [] if last else now
        for r, t in held:
            epi(r, t)

    @pl.when(n == 0)
    def _():
        run(q_epi, None, True)

    @pl.when(n == 1)
    def _():
        run(k_epi, q_epi, True)

    @pl.when(n == 2)
    def _():
        run(put, k_epi, False)


def qkv(which, sc, y, w3, b, qg, kg, cos, sin, lim, bufs):
    m = SHARD // QBM
    at = lambda i, w, s: s[w[0]] * m + i
    full = lambda *s: pl.BlockSpec(s, lambda i, n, w, s_: (0,) * len(s))
    anyspec = pl.BlockSpec(memory_space=pl.ANY)
    return pl.pallas_call(
        qkv_kernel,
        grid_spec=pltpu.PrefetchScalarGridSpec(
            num_scalar_prefetch=2, grid=(m, 3),
            in_specs=[pl.BlockSpec((QBM, D), lambda i, n, w, s: (i, 0)),
                      pl.BlockSpec((1, D, DQ), lambda i, n, w, s: (n, 0, 0)),
                      full(3, DQ), full(1, HD), full(1, HD),
                      pl.BlockSpec((QBM, HD), lambda i, n, w, s: (at(i, w, s), 0)),
                      pl.BlockSpec((QBM, HD), lambda i, n, w, s: (at(i, w, s), 0)),
                      full(8, HD), anyspec, anyspec, anyspec],
            out_specs=[pl.BlockSpec((QBM, DQ), lambda i, n, w, s: (at(i, w, s), 0)),
                       pl.BlockSpec((QBM, DQ), lambda i, n, w, s: (at(i, w, s), 0)),
                       pl.BlockSpec((DQ, QBM), lambda i, n, w, s: (0, at(i, w, s))),
                       full(8, HD)],
            scratch_shapes=[pltpu.VMEM((SROW, SUB), F32)] * 2),
        out_shape=[jax.ShapeDtypeStruct((SEQ, DQ), BF), jax.ShapeDtypeStruct((SEQ, DQ), BF),
                   jax.ShapeDtypeStruct((DQ, SEQ), BF), jax.ShapeDtypeStruct((8, HD), F32)],
        input_output_aliases={10: 0, 11: 1, 12: 2}, compiler_params=params(),
        cost_estimate=cost(2 * SHARD * D * 3 * DQ, SHARD * D * 2 + 3 * D * DQ * 2), name="qkv")(
            which, sc, y, w3, b, qg, kg, cos, sin, lim, *bufs)


BQ = SHARD
BK = 512


def attn_kernel(head_ref, which_ref, row_ref, sc_ref, lim_ref, q_ref, k_ref, vt_ref, *refs):
    o_ref, flag_ref = refs[-2:]
    txt_len = sc_ref[4]

    @pl.when(pl.program_id(0) == 0)
    def _():
        flag_ref[0] = (jnp.max(lim_ref[...]) <= 4096.0).astype(jnp.int32)

    bq = q_ref.shape[0]
    nk = SEQ // BK
    last = BK - TXT
    first_row = sc_ref[which_ref[pl.program_id(0)]] * bq
    has_pad = jnp.logical_and(first_row + bq == SEQ, txt_len < TXT)

    def scores(j):
        return lax.dot_general(k_ref[pl.ds(j * BK, BK), :], q_ref[...], NT, preferred_element_type=F32)

    def key_ok():
        return lax.broadcasted_iota(jnp.int32, (BK, 1), 0) < last + txt_len

    def finish(acc, l):
        o = acc * (1.0 / l)
        o_ref[...] = o.T.astype(BF)

        @pl.when(has_pad)
        def _():
            last_q = pl.ds(bq - TXT, TXT)
            s = lax.dot_general(k_ref[pl.ds(VID, TXT), :], q_ref[last_q, :], NT, preferred_element_type=F32)
            pad_key = lax.broadcasted_iota(jnp.int32, (TXT, 1), 0) >= txt_len
            s = jnp.where(pad_key, s, -1e30)
            p = jnp.exp2(s - jnp.max(s, axis=0, keepdims=True))
            lp = jnp.sum(p, axis=0, keepdims=True)
            ap = jnp.dot(vt_ref[:, pl.ds(VID, TXT)], p.astype(BF), preferred_element_type=F32)
            row = lax.broadcasted_iota(jnp.int32, (TXT, 1), 0)
            o_ref[last_q, :] = jnp.where(row < txt_len, o_ref[last_q, :].astype(F32), (ap * (1.0 / lp)).T).astype(BF)

    @pl.when(flag_ref[0] == 1)
    def _():
        acc = jnp.zeros((HD, bq), F32)
        l = jnp.zeros((1, bq), F32)
        s = scores(0)
        for j in range(nk):
            nxt = scores(j + 1) if j + 1 < nk else None
            p = jnp.exp2(s)
            if j == nk - 1:
                p = jnp.where(key_ok(), p, 0.0)
            l = l + jnp.sum(p, axis=0, keepdims=True)
            acc = acc + jnp.dot(vt_ref[:, pl.ds(j * BK, BK)], p.astype(BF), preferred_element_type=F32)
            s = nxt
        finish(acc, l)

    @pl.when(flag_ref[0] == 0)
    def _():
        def step(j, carry):
            m, l, acc = carry
            at = pl.multiple_of(j * BK, BK)
            s = lax.dot_general(k_ref[pl.ds(at, BK), :], q_ref[...], NT, preferred_element_type=F32)
            s = jnp.where(jnp.logical_or(key_ok(), j < nk - 1), s, -1e30)
            mn = jnp.maximum(m, jnp.max(s, axis=0, keepdims=True))
            p = jnp.exp2(s - mn)
            a = jnp.exp2(m - mn)
            l = l * a + jnp.sum(p, axis=0, keepdims=True)
            acc = acc * a + jnp.dot(vt_ref[:, pl.ds(at, BK)], p.astype(BF), preferred_element_type=F32)
            return mn, l, acc

        init = (jnp.full((1, bq), -1e30, F32), jnp.zeros((1, bq), F32), jnp.zeros((HD, bq), F32))
        _, l, acc = lax.fori_loop(0, nk, step, init)
        finish(acc, l)


def attend(pairs, blocks, sc, lim, q, k, vt, into=None):
    n = len(pairs)
    head, which, row = (np.array(v, np.int32) for v in zip(*(pairs + [pairs[-1]] * (16 - n))))
    in_specs = [pl.BlockSpec((8, HD), lambda i, h, w, r, s: (0, 0)),
                pl.BlockSpec((BQ, HD), lambda i, h, w, r, s: (s[w[i]], h[i])),
                pl.BlockSpec((SEQ, HD), lambda i, h, w, r, s: (0, h[i])),
                pl.BlockSpec((HD, SEQ), lambda i, h, w, r, s: (h[i], 0))]
    args = [head, which, row, sc, lim, q, k, vt]
    if into is not None:
        in_specs.append(pl.BlockSpec(memory_space=pl.ANY))
        args.append(into)
    return pl.pallas_call(
        attn_kernel,
        grid_spec=pltpu.PrefetchScalarGridSpec(
            num_scalar_prefetch=4, grid=(n,), in_specs=in_specs,
            out_specs=pl.BlockSpec((BQ, HD), lambda i, h, w, r, s: (r[i], h[i])),
            scratch_shapes=[pltpu.SMEM((1,), jnp.int32)]),
        out_shape=jax.ShapeDtypeStruct((blocks * BQ, DQ), BF), input_output_aliases={} if into is None else {8: 0},
        compiler_params=params(), cost_estimate=cost(6 * n * BQ * SEQ * HD, 4 * HD * n * (SEQ + BQ)), name="attend")(*args)


KC = 512
BN = 512
NL = BN // HD
NK = D // KC
NX = D // HD
NJ = D // BN
NP = 3
TILES = tuple((r, 256) for r in range(0, SHARD, 256))


def gelu(u):
    h = 0.5 * u
    t = jnp.tanh(u * (0.7978845608028654 + 0.03567740813636141 * (u * u)))
    return (h * t + h).astype(BF)


def dot(a, b):
    return jnp.dot(jnp.concatenate(a, axis=1), jnp.concatenate(b, axis=1), preferred_element_type=F32)


def tiled(product, store):
    held = None
    for tile in TILES:
        now = product(tile)
        if held is not None:
            store(*held)
        held = (tile, now)
    store(*held)


def started(copies):
    for c in copies:
        c.start()


def waited(copies):
    for c in copies:
        c.wait()


def mlp_kernel(fused, *refs):
    if fused:
        sc_ref, y0_ref, y1_ref, wa_ref, wb_ref, b_ref, o_ref, *cut_refs = refs[:7 + NP]
    else:
        y0_ref, y1_ref, wa_ref, wb_ref, b_ref, o_ref = refs[:6]
        cut_refs = []
    xs, ws, sx, sw, sf, *more = refs[6 + len(cut_refs) + (1 if fused else 0):]
    i = pl.program_id(0)
    s = pl.program_id(1)
    steps = 2 * NJ if fused else NJ
    slot = (i * steps + s) % 2

    def copy_x(y_ref, at, c):
        return [pltpu.make_async_copy(y_ref.at[:, pl.ds(x * HD, HD)], xs.at[at, x], sx.at[at, x]) for x in range(c * NL, c * NL + NL)]

    def columns(col, n):
        return pl.ds(pl.multiple_of(col * BN + n * HD, HD), HD)

    def copy_w(w_ref, col, at):
        return [pltpu.make_async_copy(w_ref.at[:, columns(col, n)], ws.at[at, n], sw.at[at, n]) for n in range(NL)]

    def first_w(c):
        k = pl.ds(c * KC, KC)
        return [pltpu.make_async_copy(wa_ref.at[k, columns(0, n)], ws.at[0, n, k], sf.at[c, n]) for n in range(NL)]

    first = jnp.logical_and(i == 0, s == 0)
    half = wa_ref.shape[1] // BN

    @pl.when(first)
    def _():
        for c in range(NK):
            started(copy_x(y0_ref, 0, c))
            started(first_w(c))

    @pl.when(s + 1 < half)
    def _():
        started(copy_w(wa_ref, s + 1, 1 - slot))

    @pl.when(jnp.logical_and(s + 1 >= half, s + 1 < steps))
    def _():
        started(copy_w(wb_ref, s + 1 - half, 1 - slot))

    @pl.when(jnp.logical_and(s + 1 == steps, i == 0))
    def _():
        started(copy_w(wa_ref, 0, 1 - slot))

    @pl.when(jnp.logical_and(s == 1, i == 0))
    def _():
        for c in range(NK):
            started(copy_x(y1_ref, 1, c))

    @pl.when(jnp.logical_and(s == 0, i == 1))
    def _():
        for c in range(NK):
            waited(copy_x(y1_ref, 1, c))

    if fused:
        qs, sq_in, sq_out = more[1:]
        t = i * steps + s
        size = D // NP // 4
        rows = lambda p: pl.ds(pl.multiple_of(p * (D // NP) + sc_ref[5] * size, size), size)
        cut_in = lambda: [pltpu.make_async_copy(wb_ref.at[rows(p), :], qs.at[p], sq_in.at[p]) for p in range(NP)]
        cut_out = lambda: [pltpu.make_async_copy(qs.at[p], cut_refs[p], sq_out.at[p]) for p in range(NP)]

        @pl.when(t == 2)
        def _():
            started(cut_in())

        @pl.when(t == 5)
        def _():
            waited(cut_in())
            started(cut_out())

        @pl.when(t == 9)
        def _():
            waited(cut_out())

    bias = b_ref[:, pl.ds(pl.multiple_of(jnp.minimum(s, NJ - 1) * BN, BN), BN)]

    def put(tile, u):
        g = gelu(u + bias)
        if fused:
            for n in range(NL):
                more[0][s * NL + n, pl.ds(*tile), :] = g[:, n * HD:(n + 1) * HD]
        else:
            o_ref[pl.ds(*tile), :] = g

    @pl.when(first)
    def _():
        acc = [None] * len(TILES)
        for c in range(NK):
            waited(copy_x(y0_ref, 0, c))
            waited(first_w(c))
            w = [ws[0, n, pl.ds(c * KC, KC), :] for n in range(NL)]
            for n, tile in enumerate(TILES):
                r = dot([xs[0, x, pl.ds(*tile), :] for x in range(c * NL, c * NL + NL)], w)
                acc[n] = r if c == 0 else acc[n] + r
        for tile, u in zip(TILES, acc):
            put(tile, u)

    @pl.when(jnp.logical_not(first))
    def _():
        waited(copy_w(wa_ref, 0, slot))

    def weights():
        return [ws[slot, n] for n in range(NL)]

    @pl.when(jnp.logical_and(jnp.logical_not(first), s < NJ))
    def _():
        tiled(lambda tile: dot([xs[i, x, pl.ds(*tile), :] for x in range(NX)], weights()), put)

    if fused:
        @pl.when(s >= NJ)
        def _():
            def store(tile, r):
                o_ref[pl.ds(*tile), :] = r

            tiled(lambda tile: dot([more[0][x, pl.ds(*tile), :] for x in range(NX)], weights()), store)


def mlp(fused, y0, y1, wa, wb, b, sc=None):
    steps = 2 * NJ if fused else NJ
    anyspec = pl.BlockSpec(memory_space=pl.ANY)
    dma = pltpu.SemaphoreType.DMA
    if fused:
        omap = lambda i, s: (jnp.where(s >= NJ, i, 0), jnp.where(s >= NJ, s - NJ, jnp.where(i == 0, 0, NJ - 1)))
    else:
        omap = lambda i, s: (i, s)
    in_specs = [anyspec] * 4 + [pl.BlockSpec((1, D), lambda i, s: (0, 0))]
    out_specs = [pl.BlockSpec((SHARD, BN), omap)]
    out_shape = [jax.ShapeDtypeStruct((CHIP, D), F32 if fused else BF)]
    scratch = [pltpu.VMEM((2, NX, SHARD, HD), BF), pltpu.VMEM((2, NL, D, HD), BF), dma((2, NX)), dma((2, NL)), dma((NK, NL))]
    args = [y0, y1, wa, wb, b]
    if fused:
        size = D // NP // 4
        in_specs.insert(0, pl.BlockSpec(memory_space=pltpu.SMEM))
        args.insert(0, sc)
        out_specs += [anyspec] * NP
        out_shape += [jax.ShapeDtypeStruct((size, D), BF)] * NP
        scratch += [pltpu.VMEM((NX, SHARD, HD), BF), pltpu.VMEM((NP, size, D), BF), dma((NP,)), dma((NP,))]
    return pl.pallas_call(
        functools.partial(mlp_kernel, fused), grid=(2, steps), in_specs=in_specs, out_specs=out_specs, out_shape=out_shape,
        scratch_shapes=scratch, compiler_params=params(63),
        cost_estimate=cost(2 * CHIP * D * steps * BN, CHIP * D * 8), name="mlp")(*args)


KO = D + 2 * DQ
OCHUNKS = tuple((c * KC, KC) for c in range(NK)) + ((D, DQ), (D + DQ, DQ))


def out_kernel(final, first_row, a0_row, *refs):
    m_ref, *w_refs, a0_ref, a1_ref, v0_ref, v1_ref, p_ref = refs[:6 + NP]
    extra = refs[6 + NP:10 + NP] if final else ()
    o_ref, xs, ws, ps, sx, sw, sp = refs[6 + NP + len(extra):6 + NP + len(extra) + 7]
    j = pl.program_id(0)
    slot = j % 2
    if final:
        recv_ref, t_ref, gate_ref, bo_ref = extra
        rs, ts, sr, st = refs[-4:]

    def copy_x(c):
        k, n = OCHUNKS[c]
        cs = []
        for x in range(k // HD, (k + n) // HD):
            if k < D:
                s = m_ref.at[pl.ds(first_row, SHARD), pl.ds(x * HD, HD)]
            else:
                a_ref, row = (a0_ref, a0_row) if k == D else (a1_ref, 0)
                s = a_ref.at[pl.ds(row, SHARD), pl.ds(x * HD - k, HD)]
            cs.append(pltpu.make_async_copy(s, xs.at[x], sx.at[x]))
        return cs

    def copy_w(c, col, at):
        k, n = OCHUNKS[c]
        piece = D // NP
        w_ref, top = (w_refs[k // piece], k % piece) if k < D else (v0_ref, 0) if k == D else (v1_ref, 0)
        cols = lambda l: pl.ds(pl.multiple_of(col * BN + l * HD, HD), HD)
        return [pltpu.make_async_copy(w_ref.at[pl.ds(top, n), cols(l)], ws.at[at, l, pl.ds(k, n)], sw.at[at, c, l]) for l in range(NL)]

    def copy_tail(col, at):
        col = pl.ds(pl.multiple_of(col * BN, BN), BN)
        cs = [pltpu.make_async_copy(p_ref.at[pl.ds(first_row, SHARD), col], ps.at[at], sp.at[at])]
        if final:
            cs += [pltpu.make_async_copy(recv_ref.at[:, col], rs.at[at], sr.at[at]), pltpu.make_async_copy(t_ref.at[:, col], ts.at[at], st.at[at])]
        return cs

    chunks = range(len(OCHUNKS))

    @pl.when(j == 0)
    def _():
        for c in chunks:
            started(copy_x(c))
            started(copy_w(c, 0, 0))
        started(copy_tail(0, 0))

    @pl.when(j + 1 < NJ)
    def _():
        for c in chunks:
            started(copy_w(c, j + 1, 1 - slot))
        started(copy_tail(j + 1, 1 - slot))

    def store(tile, acc):
        rows = pl.ds(*tile)
        acc = acc + ps[slot, rows, :]
        if final:
            acc = ts[slot, rows, :].astype(F32) + gate_ref[...] * (acc + rs[slot, rows, :] + bo_ref[...])
        o_ref[rows, :] = acc.astype(o_ref.dtype)

    @pl.when(j == 0)
    def _():
        acc = [None] * len(TILES)
        for c in chunks:
            waited(copy_x(c))
            waited(copy_w(c, 0, 0))
            k, n = OCHUNKS[c]
            w = [ws[0, l, pl.ds(k, n), :] for l in range(NL)]
            for a, tile in enumerate(TILES):
                r = dot([xs[x, pl.ds(*tile), :] for x in range(k // HD, (k + n) // HD)], w)
                acc[a] = r if c == 0 else acc[a] + r
        waited(copy_tail(0, 0))
        for tile, r in zip(TILES, acc):
            store(tile, r)

    @pl.when(j > 0)
    def _():
        for c in chunks:
            waited(copy_w(c, 0, slot))
        waited(copy_tail(0, slot))
        tiled(lambda tile: dot([xs[x, pl.ds(*tile), :] for x in range(KO // HD)], [ws[slot, l] for l in range(NL)]), store)


def out_rows(first_row, a0_row, m, wms, a0, a1, v0, v1, part, tail=None):
    anyspec = pl.BlockSpec(memory_space=pl.ANY)
    vec = pl.BlockSpec((1, BN), lambda j: (0, j))
    final = tail is not None
    nc = len(OCHUNKS)
    dma = pltpu.SemaphoreType.DMA
    scratch = [pltpu.VMEM((KO // HD, SHARD, HD), BF), pltpu.VMEM((2, NL, KO, HD), BF), pltpu.VMEM((2, SHARD, BN), F32),
               dma((KO // HD,)), dma((2, nc, NL)), dma((2,))]
    if final:
        scratch += [pltpu.VMEM((2, SHARD, BN), F32), pltpu.VMEM((2, SHARD, BN), BF), dma((2,)), dma((2,))]
    return pl.pallas_call(
        functools.partial(out_kernel, final, first_row, a0_row), grid=(NJ,),
        in_specs=[anyspec] * (6 + NP) + ([anyspec, anyspec, vec, vec] if final else []),
        out_specs=pl.BlockSpec((SHARD, BN), lambda j: (0, j)),
        out_shape=jax.ShapeDtypeStruct((SHARD, D), BF if final else F32), scratch_shapes=scratch, compiler_params=params(),
        cost_estimate=cost(2 * SHARD * KO * D, SHARD * D * 14), name="out_rows")(m, *wms, a0, a1, v0, v1, part, *(tail or ()))


def after(v, *deps):
    return lax.optimization_barrier((v,) + deps)[0]


def solution(mesh):
    def local_step(tokens, cond_vec, txt_len, grid_hw, w_mod, b_mod, w_qkv, b_qkv, q_gain, k_gain,
                   w_mlp_in, b_mlp_in, w_out_attn, w_out_mlp, b_out):
        tp = lax.axis_index('tp')
        dp = lax.axis_index('dp')
        own = tp % 2
        x = tokens[0]

        def swap_x(v):
            return lax.ppermute(v, 'tp', X_PAIRS)

        def swap_c(v):
            return lax.ppermute(v, 'tp', C_PAIRS)

        gather = lambda v: lax.all_gather(v, 'dp', axis=0, tiled=True)

        q4 = D // 4
        split = D // 3
        hop_in = [swap_x(lax.dynamic_slice(w_mlp_in, (dp * q4, lo), (q4, n)))
                  for lo, n in ((0, split), (split, D - split))]
        b_in_o = swap_x(b_mlp_in)[None]

        sib = tp + 1 - 2 * own
        rem = (tp + 2) % 4
        remsib = (sib + 2) % 4
        sc = jnp.stack([tp, sib, rem, remsib, txt_len[0], dp]).astype(jnp.int32)
        OWN, SIB, REM, REMSIB = (np.full((1,), i, np.int32) for i in range(4))

        qg = q_gain[None]
        kg = k_gain[None]
        y, cos, sin, gate, lim, *bufs = prep(grid_hw, cond_vec, w_mod, b_mod, x, qg, kg)
        y_sib = swap_c(y)
        y_rem = swap_x(y)
        tabs = (jnp.transpose(w_qkv, (1, 0, 2)), b_qkv, qg, kg, cos, sin)

        w_in_o0 = gather(after(hop_in[0], y))
        *bufs, lim = qkv(OWN, sc, y, *tabs, lim, bufs)
        *bufs, lim = qkv(SIB, sc, y_sib, *tabs, lim, bufs)
        w_in_o1 = gather(after(hop_in[1], lim))
        part, *cut = mlp(True, y, after(y_sib, lim), w_mlp_in, w_out_mlp, b_mlp_in[None], sc)
        hop_out = [swap_x(c) for c in cut]
        w_att_o = swap_x(w_out_attn)
        m_oth, = mlp(False, y, y_sib, w_in_o0, w_in_o1, b_in_o)
        y_rem = after(y_rem, m_oth)
        y_remsib = swap_c(y_rem)
        *bufs, lim = qkv(REM, sc, y_rem, *tabs, lim, bufs)
        w_out_o = [gather(after(hop_out[0], lim))]
        q, k, vt, lim = qkv(REMSIB, sc, y_remsib, *tabs, lim, bufs)
        w_out_o.append(gather(after(hop_out[1], lim)))

        att_r0 = attend([(h, 3, 0) for h in range(NH)], 1, sc, lim, q, k, vt)
        att_b0 = swap_x(att_r0)
        w_out_o.append(gather(after(hop_out[2], att_r0)))
        att_r1 = attend([(h, 2, 0) for h in range(NH)], 1, after(sc, att_r0), lim, q, k, vt)
        att_b1 = swap_x(att_r1)
        some = NH // 2
        att_a = attend([(h, 1, 0) for h in range(NH)] + [(h, 0, 1) for h in range(some)], 2, after(sc, att_r1), lim, q, k, vt)

        wms = tuple(w_out_o)
        weights = (w_out_attn, w_att_o, part)
        sib_part = out_rows(SHARD, 0, m_oth, wms, att_a, att_b0, *weights)
        recv = swap_c(sib_part)
        att_a = attend([(h, 0, 1) for h in range(some, NH)], 2, after(sc, sib_part), lim, q, k, vt, after(att_a, sib_part))
        out = out_rows(0, SHARD, m_oth, wms, att_a, att_b1, *weights, (recv, x, gate, b_out[None]))
        return out[None]

    in_specs = (P('dp', 'tp', None), P('dp', None), P('dp'), P('dp', None), P(None, None), P(None), P(None, None, 'tp'), P(None, 'tp'), P(None), P(None), P(None, 'tp'), P('tp'), P('tp', None), P('tp', None), P(None))
    return jax.shard_map(local_step, mesh=mesh, in_specs=in_specs, out_specs=P('dp', 'tp', None), check_vma=False)
```
